128 devices in a mesh: dp: 16 (over x, z_lo, core), tensor: 8 (over y, z_hi).
Axes of the slice: x: 4, y: 4, z: 4 (z_hi: 2, z_lo: 2; z = z_hi * 2 + z_lo), core: 2. Of those that a mesh axis runs over, the one named last changes fastest.
Arguments:
- activations: bfloat16 [6144, 16384], P(('dp', 'tensor')), may hold values from -6 to 6
- out_grad: bfloat16 [6144, 16384], P('dp', 'tensor'), may hold values from -0.1875 to 0.1875
- block_ids: int32 [8, 12], replicated, may hold values from 0 to 127, as said below
- owner_map: int32 [16, 4], replicated, may hold values from 0 to 1, as said below
- master: float32 [1024, 16384], P('dp', 'tensor'), may hold values from -3 to 3
- moment: float32 [1024, 16384], P('dp', 'tensor'), may hold values from -3 to 3
- second: float32 [1024, 16384], P('dp', 'tensor'), may hold values from 0.01 to 2
Outputs:
- new_master: float32 [1024, 16384], P('dp', 'tensor')
- new_moment: float32 [1024, 16384], P('dp', 'tensor')
- new_second: float32 [1024, 16384], P('dp', 'tensor')
- hot_weights: bfloat16 [1024, 16384], P('dp')
- cold_recv: float32 [8192, 16384], P('dp', 'tensor')
The draws below stay inside these ranges and needn't reach their ends.
Inputs may be any that keep to these rules, and one draw needn't show every extreme that they name: `block_ids`: the 12 block numbers in a row are distinct. `owner_map`: each row has between 1 and 3 ones; some row has exactly 3 ones and some row exactly 1.
All inputs are finite; a program needn't handle non-finite values.
Results may differ from the reference program's by a relative error of at most 0.006.
Values may be sent and summed in bfloat16 or wider, within the bound.
A program may use at most 128 MiB of HBM per device.

```python
import math
import jax
import jax.numpy as jnp
from jax import lax

D = 16384
QO = 16384
BLOCK = 128
HOT = 8
COLD = 4
MOSTC = 3
TOK = 384
TOKENS = 6144
HOTR = 1024
N_DP = 16
N_TENSOR = 8


def draw_block_ids(key, part):
    keys = jax.random.split(jax.random.fold_in(key, 11), N_TENSOR)
    rows = jax.vmap(lambda single: jax.random.permutation(single, D // BLOCK)[:HOT + COLD])(keys)
    return rows.astype(jnp.int32)


def draw_owner_map(key, part):
    base = jax.random.fold_in(key, 23)
    first, second_key, third = jax.random.split(base, 3)
    counts = jax.random.randint(first, (N_DP,), COLD - MOSTC, MOSTC + 1)
    chosen = jax.random.permutation(second_key, N_DP)
    counts = counts.at[chosen[0]].set(MOSTC).at[chosen[1]].set(COLD - MOSTC)
    ranks = jax.vmap(lambda single: jax.random.permutation(single, COLD))(jax.random.split(third, N_DP))
    return (ranks < counts[:, None]).astype(jnp.int32)


def shard_levels(rng, shape, cuts, low, high):
    loudness, own = 1.0, jax.random.fold_in(rng, 6)
    for position, parts in cuts:
        draws = jnp.exp(jax.random.uniform(jax.random.fold_in(own, position), (parts,), jnp.float32, low / len(cuts), high / len(cuts)))
        loudness = loudness * jnp.repeat(draws, shape[position] // parts).reshape([-1 if axis == position else 1 for axis in range(len(shape))])
    return loudness


def bell_draw(own_key, extent, deviation, limit, shards=(), kind=jnp.bfloat16):
    factor_of = shard_levels(own_key, extent, shards, -0.22, 0.18) if shards else 1.0
    entries = jax.random.normal(own_key, extent, jnp.float32) * deviation * factor_of
    return jnp.minimum(jnp.maximum(entries, -limit), limit).astype(kind)


def setup_inputs(seed: int = 0) -> dict:
    streams_of = jax.random.split(jax.random.key(seed), 8)
    activations = bell_draw(streams_of[0], (TOKENS, D), 1.0, 6.0, ((0, 128),))
    out_grad = bell_draw(streams_of[1], (TOKENS, QO), (1.0 / TOKENS ** 0.5), 0.1875, ((0, 16), (1, 8)))
    block_ids = draw_block_ids(jax.random.fold_in(streams_of[7], 71), 0)
    owner_map = draw_owner_map(jax.random.fold_in(streams_of[7], 71), 0)
    master = bell_draw(streams_of[4], (HOTR, QO), 0.5, 3.0, ((0, 16), (1, 8)), jnp.float32)
    moment = bell_draw(streams_of[5], (HOTR, QO), 0.5, 3.0, ((0, 16), (1, 8)), jnp.float32)
    second = jnp.clip(jnp.exp(math.log(2.0) - 5.2983174 * jax.random.uniform(streams_of[6], (HOTR, QO), jnp.float32) ** shard_levels(streams_of[6], (HOTR, QO), ((0, 16), (1, 8)), -0.2, 0.2)), 0.01, 2.0)
    return {"activations": activations, "out_grad": out_grad, "block_ids": block_ids, "owner_map": owner_map, "master": master, "moment": moment, "second": second}


BETA_ONE = 0.9
BETA_TWO = 0.95
ADAM_EPS = 1e-08
LEARN_RATE = 0.01
DECAY = 0.1
CORRECT_ONE = 1.0 - 0.9 ** 10
CORRECT_TWO = 1.0 - 0.95 ** 10

def pick_blocks(tok_rows, block_row):
    shaped = tok_rows.reshape(tok_rows.shape[0], D // BLOCK, BLOCK)
    return shaped[:, block_row, :].reshape(tok_rows.shape[0], block_row.shape[0] * BLOCK)

def reference(activations, out_grad, block_ids, owner_map, master, moment, second):
    qloc = QO // N_TENSOR
    hot_rows = HOT * BLOCK

    def per_index(carry, index):
        tok_rows = lax.dynamic_slice_in_dim(activations, index * TOK, TOK, 0)
        grad_rows = lax.dynamic_slice_in_dim(out_grad, index * TOK, TOK, 0)
        hot_list = []
        cold_list = []
        for group in range(N_TENSOR):
            chosen = pick_blocks(tok_rows, block_ids[group]).astype(jnp.float32)
            grad_cols = grad_rows[:, group * qloc:(group + 1) * qloc].astype(jnp.float32)
            product = jnp.dot(chosen.T, grad_cols, preferred_element_type=jnp.float32)
            hot_list.append(product[:hot_rows].astype(jnp.bfloat16).astype(jnp.float32))
            cold_list.append(product[hot_rows:].astype(jnp.bfloat16))
        return (carry + jnp.stack(hot_list), jnp.stack(cold_list))
    start_sum = jnp.zeros((N_TENSOR, hot_rows, qloc), jnp.float32)
    hot_sum, cold_parts = lax.scan(per_index, start_sum, jnp.arange(N_DP, dtype=jnp.int32))
    grad = hot_sum.transpose(1, 0, 2).reshape(hot_rows, QO)
    cold_parts = cold_parts.reshape(N_DP, N_TENSOR, COLD, BLOCK, qloc)
    from_prev = jnp.roll(cold_parts, 1, axis=0)
    from_next = jnp.roll(cold_parts, -1, axis=0)
    prev_owner = jnp.roll(owner_map, 1, axis=0)[:, None, :, None, None]
    next_owner = jnp.roll(owner_map, -1, axis=0)[:, None, :, None, None]
    total = jnp.where(prev_owner == 1, from_prev.astype(jnp.float32), 0.0)
    total = total + jnp.where(next_owner == 0, from_next.astype(jnp.float32), 0.0)
    cold_recv = total.transpose(0, 2, 3, 1, 4).reshape(N_DP * COLD * BLOCK, QO)
    new_moment = BETA_ONE * moment + (1.0 - BETA_ONE) * grad
    new_second = BETA_TWO * second + (1.0 - BETA_TWO) * grad * grad
    update = new_moment / CORRECT_ONE / (jnp.sqrt(new_second / CORRECT_TWO) + ADAM_EPS)
    new_master = master - LEARN_RATE * (update + DECAY * master)
    hot_weights = new_master.astype(jnp.bfloat16)
    return (new_master, new_moment, new_second, hot_weights, cold_recv)
```

```python
import jax
import jax.numpy as jnp
from jax import lax
from jax.experimental import pallas as pl
from jax.experimental.pallas import tpu as pltpu
from jax.sharding import PartitionSpec as P

D = 16384
BLOCK = 128
HOT = 8
COLD = 4
SENT = 3
HALF = BLOCK // 2
CHUNKS = 4
EARLY = 2
MIDDLE = 3

BETA_ONE = 0.9
BETA_TWO = 0.95
ADAM_EPS = 1e-08
LEARN_RATE = 0.01
DECAY = 0.1
CORRECT_ONE = 1.0 - 0.9**10
CORRECT_TWO = 1.0 - 0.95**10

OFFSETS = ((2, 1), (1, 1), (3, 1), (0, 1), (2, 0), (1, 0), (3, 0))
CONTRACT = (((1,), (0,)), ((), ()))
F32 = jnp.float32
BF16 = jnp.bfloat16


def slots(own, index):
    ones = [own[index, k] for k in range(COLD)]
    seen, places = jnp.int32(0), []
    for k in range(COLD):
        places.append(seen)
        seen = seen + ones[k]
    places = [jnp.where(ones[k] == 1, places[k], seen + k - places[k]) for k in range(COLD)]
    return ones, places


def pick(ids, own, act, hot, cold):
    _, mine = slots(own, lax.axis_index("dp"))

    def columns(block):
        return act[:, pl.ds(pl.multiple_of(block * BLOCK, BLOCK), BLOCK)]

    def group_step(group, carry):
        for k in range(HOT):
            hot[group, :, k * BLOCK : (k + 1) * BLOCK] = columns(ids[group, k])
        for slot in range(COLD):
            block = jnp.int32(0)
            for k in range(COLD):
                block = block + jnp.where(mine[k] == slot, ids[group, HOT + k], 0)
            cold[group, :, slot * BLOCK : (slot + 1) * BLOCK] = columns(block)
        return carry

    lax.fori_loop(0, hot.shape[0], group_step, 0)


def kernel(
    send_hot, send_cold, og_h, ma_h, mo_h, se_h,
    oma_h, omo_h, ose_h, ohw_h, prev_h, next_h,
    og, state, hot_in, cold_in,
    prod, pair, quads, a_in, b_in, z_out, z_in, weights,
    part0, part1, part2, part3, load_sem, out_sem,
    hs_sem, hr_sem, cs_sem, cr_sem, ds_sem, dr_sem, as_sem, ar_sem, bs_sem, br_sem,
    zs_sem, zr_sem, ps_sem, pr_sem, ns_sem, nr_sem, gs_sem, gr_sem,
):
    rows, qlocal = send_hot.shape[1], og.shape[1]
    width = qlocal // CHUNKS
    i = lax.axis_index("dp")
    t = lax.axis_index("tensor")
    x, zl, c = lax.div(i, 4), lax.rem(lax.div(i, 2), 2), lax.rem(i, 2)
    y, zh = lax.div(t, 2), lax.rem(t, 2)

    def device(x_, zl_, c_):
        return ((x_ * 2 + zl_) * 2 + c_, t)

    def tensor(dy, dz):
        return lax.rem(y + dy, 4) * 2 + lax.rem(zh + dz, 2)

    right, left = device(lax.rem(x + 1, 4), zl, c), device(lax.rem(x + 3, 4), zl, c)
    mate, across = device(x, zl, 1 - c), device(x, 1 - zl, c)
    after, before = (lax.rem(i + 1, 16), t), (lax.rem(i + 15, 16), t)
    far = (lax.rem(i + 15 + 2 * c, 16), t)

    def remote(src, dst, send, recv, to):
        return pltpu.make_async_remote_copy(
            src_ref=src, dst_ref=dst, send_sem=send, recv_sem=recv, device_id=to,
            device_id_type=pl.DeviceIdType.MESH,
        )

    own_rows = pl.ds(pl.multiple_of(t * rows, rows), rows)
    loads = [
        pltpu.make_async_copy(send_hot.at[t], hot_in.at[own_rows], load_sem.at[0]),
        pltpu.make_async_copy(og_h, og, load_sem.at[1]),
        pltpu.make_async_copy(send_cold.at[t], cold_in.at[own_rows], load_sem.at[2]),
        pltpu.make_async_copy(ma_h, state.at[0], load_sem.at[3]),
        pltpu.make_async_copy(mo_h, state.at[1], load_sem.at[4]),
        pltpu.make_async_copy(se_h, state.at[2], load_sem.at[5]),
    ]
    for load in loads:
        load.start()

    barrier = pltpu.get_barrier_semaphore()
    peers = [(i, tensor(dy, dz)) for dy, dz in OFFSETS] + [right, left, mate, across, far]
    for peer in peers:
        pl.semaphore_signal(barrier, inc=1, device_id=peer, device_id_type=pl.DeviceIdType.MESH)

    pl.semaphore_wait(barrier, len(peers))

    def hot_copy(n):
        to = tensor(*OFFSETS[n])
        return remote(send_hot.at[to], hot_in.at[own_rows], hs_sem.at[n], hr_sem.at[n], (i, to))

    def cold_copy(n):
        to = tensor(*OFFSETS[n])
        return remote(send_cold.at[to], cold_in.at[own_rows], cs_sem.at[n], cr_sem.at[n], (i, to))

    for n in range(len(OFFSETS)):
        hot_copy(n).start()
    for n in range(len(OFFSETS)):
        cold_copy(n).start()
    loads[0].wait()
    loads[1].wait()
    for n in range(len(OFFSETS)):
        hot_copy(n).wait_recv()

    def mate_copy(k):
        return remote(prod.at[k, 1 - c], pair.at[k], ds_sem.at[k], dr_sem.at[k], mate)

    def hot_step(k, carry):
        dx = jnp.where(k < 2, 2, jnp.where(k < 4, 1, jnp.where(k < 6, 3, 0)))
        side = lax.rem(k, 2)
        side = jnp.where(k < 6, side, jnp.where(k == 6, 1 - zl, zl))
        block = lax.rem(x + dx, 4) * 2 + side
        picked = hot_in[:, pl.ds(pl.multiple_of(block * BLOCK, BLOCK), BLOCK)].T
        for n in range(CHUNKS):
            cols = pl.ds(n * width, width)
            got = lax.dot_general(picked, og[:, cols], CONTRACT, preferred_element_type=F32)
            got = got.astype(BF16)
            prod[k, 0, :, cols] = got[:HALF]
            prod[k, 1, :, cols] = got[HALF:]
        mate_copy(k).start()
        return carry

    lax.fori_loop(0, HOT, hot_step, 0)

    def pair_sum(k):
        mate_copy(k).wait_recv()
        return prod[k, c].astype(F32) + pair[k].astype(F32)

    a_right = remote(quads.at[0], a_in.at[0], as_sem.at[0], ar_sem.at[0], right)
    a_left = remote(quads.at[1], a_in.at[1], as_sem.at[1], ar_sem.at[1], left)
    b_right = [
        remote(quads.at[2 + k], b_in.at[k], bs_sem.at[k], br_sem.at[k], right) for k in range(2)
    ]
    b_left = [
        remote(quads.at[4 + k], b_in.at[2 + k], bs_sem.at[2 + k], br_sem.at[2 + k], left)
        for k in range(2)
    ]
    quads[0] = pair_sum(0).astype(BF16)
    a_right.start()
    quads[1] = pair_sum(1).astype(BF16)
    a_left.start()
    quads[3] = pair_sum(3).astype(BF16)
    b_right[1].start()
    quads[4] = pair_sum(4).astype(BF16)
    b_left[0].start()

    parts = (part0, part1, part2, part3)
    to_next = [
        remote(parts[n].at[0:SENT], prev_h.at[n], ps_sem.at[n], pr_sem.at[n], after)
        for n in range(CHUNKS)
    ]
    to_prev = [
        remote(parts[n].at[1 : 1 + SENT], next_h.at[n], ns_sem.at[n], nr_sem.at[n], before)
        for n in range(CHUNKS)
    ]

    def send_chunk(n):
        to_next[n].start()
        to_prev[n].start()

    loads[2].wait()
    for n in range(len(OFFSETS)):
        cold_copy(n).wait_recv()
    for n in range(CHUNKS):
        cols = pl.ds(n * width, width)
        for slot in range(COLD):
            picked = cold_in[:, slot * BLOCK : (slot + 1) * BLOCK].T
            got = lax.dot_general(picked, og[:, cols], CONTRACT, preferred_element_type=F32)
            parts[n][slot] = got.astype(BF16)
        if n < EARLY:
            send_chunk(n)

    first = pair_sum(2)
    a_right.wait_recv()
    quads[2] = (first + a_in[0].astype(F32)).astype(BF16)
    b_right[0].start()
    second = pair_sum(5)
    a_left.wait_recv()
    quads[5] = (second + a_in[1].astype(F32)).astype(BF16)
    b_left[1].start()
    for copy in b_right + b_left:
        copy.wait_recv()

    def arrived(k, side):
        return b_in[side].astype(F32) + b_in[2 + side].astype(F32)

    z_copy = remote(z_out, z_in, zs_sem, zr_sem, across)
    z_out[...] = (pair_sum(6) + arrived(6, 1 - zl)).astype(BF16)
    z_copy.start()
    for n in range(EARLY, MIDDLE):
        send_chunk(n)
    mate_copy(7).wait_recv()
    for load in loads[3:]:
        load.wait()
    z_copy.wait_recv()

    step_rows = 16

    def adam_step(k, carry):
        at = pl.ds(pl.multiple_of(k * step_rows, step_rows), step_rows)
        grad = prod[7, c, at].astype(F32) + pair[7, at].astype(F32) + z_in[at].astype(F32)
        grad = grad + b_in[zl, at].astype(F32) + b_in[2 + zl, at].astype(F32)
        master = state[0, at]
        moment = BETA_ONE * state[1, at] + (1.0 - BETA_ONE) * grad
        second = BETA_TWO * state[2, at] + (1.0 - BETA_TWO) * grad * grad
        update = moment / CORRECT_ONE / (jnp.sqrt(second / CORRECT_TWO) + ADAM_EPS)
        master = master - LEARN_RATE * (update + DECAY * master)
        state[0, at] = master
        state[1, at] = moment
        state[2, at] = second
        weights[t, at] = master.astype(BF16)
        return carry

    lax.fori_loop(0, HALF // step_rows, adam_step, 0)

    half = qlocal // 2

    def whole(slot):
        return weights.at[slot]

    def gather(n, slot, to, part=None):
        ref = weights.at[slot] if part is None else weights.at[slot, :, pl.ds(part * half, half)]
        return remote(ref, ref, gs_sem.at[n], gr_sem.at[n], (i, to))

    up, down, other = tensor(1, 0), tensor(3, 0), tensor(0, 1)
    g_up = gather(0, t, up)
    g_down = gather(1, t, down)
    g_other = gather(2, t, other)
    g_up.start()
    g_down.start()
    g_other.start()
    for n in range(MIDDLE, CHUNKS):
        send_chunk(n)

    outs = [
        pltpu.make_async_copy(state.at[0], oma_h, out_sem.at[0]),
        pltpu.make_async_copy(state.at[1], omo_h, out_sem.at[1]),
        pltpu.make_async_copy(state.at[2], ose_h, out_sem.at[2]),
    ]
    for out in outs:
        out.start()

    g_up.wait_recv()
    f_up = gather(3, tensor(3, 0), up, 0)
    f_up.start()
    g_down.wait_recv()
    f_down = gather(4, tensor(1, 0), down, 1)
    f_down.start()
    g_other.wait_recv()
    o_up = gather(5, other, up)
    o_down = gather(6, other, down)
    o_up.start()
    o_down.start()

    o_up.wait_recv()
    of_up = gather(7, tensor(3, 1), up, 0)
    of_up.start()
    o_down.wait_recv()
    of_down = gather(8, tensor(1, 1), down, 1)
    of_down.start()

    f_up.wait_recv()
    f_down.wait_recv()
    of_up.wait_recv()
    of_down.wait_recv()
    out = pltpu.make_async_copy(weights, ohw_h, out_sem.at[3])
    out.start()
    outs.append(out)
    for n in range(CHUNKS):
        to_next[n].wait_recv()
        to_prev[n].wait_recv()

    for n in range(len(OFFSETS)):
        hot_copy(n).wait_send()
        cold_copy(n).wait_send()
    for k in range(HOT):
        mate_copy(k).wait_send()
    sends = [a_right, a_left, *b_right, *b_left, z_copy, *to_next, *to_prev]
    sends += [g_up, g_down, g_other, f_up, f_down, o_up, o_down, of_up, of_down]
    for copy in sends:
        copy.wait_send()
    for out in outs:
        out.wait()


def finish(
    own, ma_h, mo_h, se_h, hw_h, prev_h, next_h, oma_h, omo_h, ose_h, ohw_h, ocold_h,
    state, weights, prev, late, stage, in_sem, cold_sem, out_sem, done_sem,
):
    i = lax.axis_index("dp")
    width = prev.shape[-1]
    qlocal = width * CHUNKS
    chunks = []
    for n in range(CHUNKS):
        chunks.append(
            (
                pltpu.make_async_copy(prev_h.at[n], prev.at[n], cold_sem.at[n, 0]),
                pltpu.make_async_copy(next_h.at[n], late.at[n], cold_sem.at[n, 1]),
            )
        )
        for copy in chunks[n]:
            copy.start()
    ins = [
        pltpu.make_async_copy(ref, state.at[k], in_sem.at[k])
        for k, ref in enumerate((ma_h, mo_h, se_h))
    ]
    ins.append(pltpu.make_async_copy(hw_h, weights, in_sem.at[3]))
    for copy in ins:
        copy.start()
    ones_prev, place_prev = slots(own, lax.rem(i + 15, 16))
    ones_next, place_next = slots(own, lax.rem(i + 1, 16))
    outs = []
    for n in range(CHUNKS):
        for copy in chunks[n]:
            copy.wait()
        for k in range(COLD):
            a = prev[n, jnp.minimum(place_prev[k], SENT - 1)].astype(F32)
            b = late[n, jnp.maximum(place_next[k] - 1, 0)].astype(F32)
            a = jnp.where(ones_prev[k] == 1, a, 0.0)
            b = jnp.where(ones_next[k] == 0, b, 0.0)
            stage[n, k * BLOCK : (k + 1) * BLOCK] = a + b
        outs.append(
            pltpu.make_async_copy(
                stage.at[n], ocold_h.at[:, pl.ds(n * width, width)], done_sem.at[n]
            )
        )
        outs[-1].start()
        if n == 0:
            for copy in ins:
                copy.wait()
            for k, ref in enumerate((oma_h, omo_h, ose_h)):
                outs.append(pltpu.make_async_copy(state.at[k], ref, out_sem.at[k]))
                outs[-1].start()
            for slot in range(8):
                outs.append(
                    pltpu.make_async_copy(
                        weights.at[slot],
                        ohw_h.at[:, pl.ds(slot * qlocal, qlocal)],
                        out_sem.at[3 + slot],
                    )
                )
                outs[-1].start()
    for out in outs:
        out.wait()


def per_device(activations, out_grad, block_ids, owner_map, master, moment, second):
    rows, tokens, qlocal = activations.shape[0], out_grad.shape[0], out_grad.shape[1]
    width = qlocal // CHUNKS
    partners = len(OFFSETS)
    dma = pltpu.SemaphoreType.DMA
    any_space = pl.BlockSpec(memory_space=pl.ANY)
    smem = pl.BlockSpec(memory_space=pltpu.SMEM)
    like = jax.ShapeDtypeStruct
    arrived = like((CHUNKS, SENT, BLOCK, width), BF16)
    states = (like(master.shape, F32),) * 3
    vmem = pl.BlockSpec(memory_space=pltpu.VMEM)
    chosen = pl.pallas_call(
        pick,
        name="pick",
        out_shape=(like((8, rows, HOT * BLOCK), BF16), like((8, rows, COLD * BLOCK), BF16)),
        in_specs=[smem, smem, vmem],
        out_specs=(vmem, vmem),
        compiler_params=pltpu.CompilerParams(vmem_limit_bytes=16 * 1024 * 1024),
    )(block_ids, owner_map, activations)
    gathered = pl.pallas_call(
        kernel,
        name="exchange",
        out_shape=(*states, like((8, HALF, qlocal), BF16), arrived, arrived),
        in_specs=[any_space] * 6,
        out_specs=(any_space,) * 6,
        scratch_shapes=[
            pltpu.VMEM((tokens, qlocal), BF16),
            pltpu.VMEM((3, HALF, qlocal), F32),
            pltpu.VMEM((tokens, HOT * BLOCK), BF16),
            pltpu.VMEM((tokens, COLD * BLOCK), BF16),
            pltpu.VMEM((HOT, 2, HALF, qlocal), BF16),
            pltpu.VMEM((HOT, HALF, qlocal), BF16),
            pltpu.VMEM((6, HALF, qlocal), BF16),
            pltpu.VMEM((2, HALF, qlocal), BF16),
            pltpu.VMEM((4, HALF, qlocal), BF16),
            pltpu.VMEM((HALF, qlocal), BF16),
            pltpu.VMEM((HALF, qlocal), BF16),
            pltpu.VMEM((8, HALF, qlocal), BF16),
            *[pltpu.VMEM((COLD, BLOCK, width), BF16)] * CHUNKS,
            dma((6,)),
            dma((4,)),
            *[dma((partners,))] * 4,
            *[dma((HOT,))] * 2,
            *[dma((2,))] * 2,
            *[dma((4,))] * 2,
            *[dma] * 2,
            *[dma((CHUNKS,))] * 4,
            *[dma((9,))] * 2,
        ],
        compiler_params=pltpu.CompilerParams(
            collective_id=0, has_side_effects=True, vmem_limit_bytes=40 * 1024 * 1024
        ),
    )(*chosen, out_grad, master, moment, second)
    return pl.pallas_call(
        finish,
        name="finish",
        out_shape=(
            *states,
            like((HALF, 8 * qlocal), BF16),
            like((COLD * BLOCK, qlocal), F32),
        ),
        in_specs=[smem] + [any_space] * 6,
        out_specs=(any_space,) * 5,
        scratch_shapes=[
            pltpu.VMEM((3, HALF, qlocal), F32),
            pltpu.VMEM((8, HALF, qlocal), BF16),
            pltpu.VMEM(arrived.shape, BF16),
            pltpu.VMEM(arrived.shape, BF16),
            pltpu.VMEM((CHUNKS, COLD * BLOCK, width), F32),
            dma((4,)),
            dma((CHUNKS, 2)),
            dma((11,)),
            dma((CHUNKS,)),
        ],
        compiler_params=pltpu.CompilerParams(vmem_limit_bytes=24 * 1024 * 1024),
    )(owner_map, *gathered)


def solution(mesh):
    return jax.shard_map(
        per_device,
        mesh=mesh,
        in_specs=(
            P(("dp", "tensor"), None),
            P("dp", "tensor"),
            P(),
            P(),
            P("dp", "tensor"),
            P("dp", "tensor"),
            P("dp", "tensor"),
        ),
        out_specs=(
            P("dp", "tensor"),
            P("dp", "tensor"),
            P("dp", "tensor"),
            P("dp", None),
            P("dp", "tensor"),
        ),
        check_vma=False,
    )
```

```python
import jax
import jax.numpy as jnp
from jax import lax
from jax.experimental import pallas as pl
from jax.experimental.pallas import tpu as pltpu
from jax.sharding import PartitionSpec as P

D = 16384
BLOCK = 128
HOT = 8
COLD = 4
SENT = 3
OWNED = 64
PARTS = 4
CHUNKS = 8
DIRECT = (6, 7, 8)
DIAGONAL = (2, 3, 8)

BETA_ONE = 0.9
BETA_TWO = 0.95
ADAM_EPS = 1e-08
LEARN_RATE = 0.01
DECAY = 0.1
CORRECT_ONE = 1.0 - 0.9**10
CORRECT_TWO = 1.0 - 0.95**10

OFFSETS = ((2, 1), (1, 1), (3, 1), (0, 1), (2, 0), (1, 0), (3, 0))
CONTRACT = (((1,), (0,)), ((), ()))
F32 = jnp.float32
BF16 = jnp.bfloat16


def place(i):
    return lax.div(i, 4), lax.rem(lax.div(i, 2), 2), lax.rem(i, 2)


def hot_block(k, x, zl):
    step = (2, 2, 1, 1, 3, 3, 0, 0)[k]
    side = (0, 1, 0, 1, 0, 1, 1 - zl, zl)[k]
    return lax.rem(x + step, 4) * 2 + side


def slots(own, index):
    ones = [own[k, index] for k in range(COLD)]
    seen, places = jnp.int32(0), []
    for k in range(COLD):
        places.append(seen)
        seen = seen + ones[k]
    places = [jnp.where(ones[k] == 1, places[k], seen + k - places[k]) for k in range(COLD)]
    return ones, places


def pick(ids, own, act_h, hot, cold, act, sem):
    load = pltpu.make_async_copy(act_h, act, sem)
    load.start()
    i = lax.axis_index("dp")
    x, zl, _ = place(i)
    _, mine = slots(own, i)
    load.wait()

    def columns(block):
        return act[:, pl.ds(pl.multiple_of(block * BLOCK, BLOCK), BLOCK)]

    def group_step(group, carry):
        for k in range(HOT):
            at = k % 2 * BLOCK
            hot[k // 2, group, :, at : at + BLOCK] = columns(ids[group, hot_block(k, x, zl)])
        for slot in range(COLD):
            block = jnp.int32(0)
            for k in range(COLD):
                block = block + jnp.where(mine[k] == slot, ids[group, HOT + k], 0)
            cold[group, :, slot * BLOCK : (slot + 1) * BLOCK] = columns(block)
        return carry

    lax.fori_loop(0, cold.shape[0], group_step, 0)


def exchange(
    send_hot, send_cold, og_h, ma_h, mo_h, se_h,
    oma_h, omo_h, ose_h, ohw_h, recv_h,
    og, state, hot_in, cold_in, prod, pair, quads, a_in, b_in, z_out, z_in, weights, parts,
    load_sem, out_sem, hs_sem, hr_sem, cs_sem, cr_sem, ds_sem, dr_sem, as_sem, ar_sem,
    bs_sem, br_sem, zs_sem, zr_sem, ns_sem, nr_sem, fs_sem, fr_sem, gs_sem, gr_sem,
):
    rows, qlocal = send_hot.shape[2], og.shape[1]
    width, half, quarter = qlocal // CHUNKS, qlocal // 2, qlocal // 4
    i = lax.axis_index("dp")
    t = lax.axis_index("tensor")
    x, zl, c = place(i)
    y, zh = lax.div(t, 2), lax.rem(t, 2)

    def device(x_, zl_, c_):
        return ((x_ * 2 + zl_) * 2 + c_, t)

    def tensor(dy, dz):
        return lax.rem(y + dy, 4) * 2 + lax.rem(zh + dz, 2)

    right, left = device(lax.rem(x + 1, 4), zl, c), device(lax.rem(x + 3, 4), zl, c)
    mate, across = device(x, zl, 1 - c), device(x, 1 - zl, c)
    far = (lax.rem(i + 15 + 2 * c, 16), t)

    started = []

    def remote(src, dst, send, recv, to):
        copy = pltpu.make_async_remote_copy(
            src_ref=src, dst_ref=dst, send_sem=send, recv_sem=recv, device_id=to,
            device_id_type=pl.DeviceIdType.MESH,
        )
        started.append(copy)
        return copy

    own_rows = pl.ds(pl.multiple_of(t * rows, rows), rows)
    load_og = pltpu.make_async_copy(og_h, og, load_sem.at[0])
    load_own = [
        pltpu.make_async_copy(send_hot.at[p, t], hot_in.at[p, own_rows], load_sem.at[1 + p])
        for p in range(PARTS)
    ]
    load_cold = pltpu.make_async_copy(send_cold.at[t], cold_in.at[own_rows], load_sem.at[5])
    load_state = [
        pltpu.make_async_copy(ref, state.at[k], load_sem.at[6 + k])
        for k, ref in enumerate((ma_h, mo_h, se_h))
    ]
    for load in (load_og, *load_own, load_cold, *load_state):
        load.start()

    barrier = pltpu.get_barrier_semaphore()
    peers = [(i, tensor(dy, dz)) for dy, dz in OFFSETS] + [right, left, mate, across, far]
    for peer in peers:
        pl.semaphore_signal(barrier, inc=1, device_id=peer, device_id_type=pl.DeviceIdType.MESH)
    pl.semaphore_wait(barrier, len(peers))

    hot_copies, cold_copies = [[] for _ in range(PARTS)], []
    for p in (0, 1, 2, None, 3):
        for n, offset in enumerate(OFFSETS):
            to = tensor(*offset)
            if p is None:
                src, dst = send_cold.at[to], cold_in.at[own_rows]
                copy = remote(src, dst, cs_sem.at[n], cr_sem.at[n], (i, to))
                cold_copies.append(copy)
            else:
                src, dst = send_hot.at[p, to], hot_in.at[p, own_rows]
                copy = remote(src, dst, hs_sem.at[p, n], hr_sem.at[p, n], (i, to))
                hot_copies[p].append(copy)
            copy.start()

    mate_copies = [
        remote(prod.at[p, 1 - c], pair.at[p], ds_sem.at[p], dr_sem.at[p], mate)
        for p in range(PARTS)
    ]

    def multiply(p):
        load_own[p].wait()
        for copy in hot_copies[p]:
            copy.wait_recv()
        picked = hot_in[p].T
        for n in range(4):
            cols = pl.ds(n * quarter, quarter)
            got = lax.dot_general(picked, og[:, cols], CONTRACT, preferred_element_type=F32)
            got = got.astype(BF16)
            for k in range(2):
                for core in range(2):
                    at = k * BLOCK + core * OWNED
                    prod[p, core, k, :, cols] = got[at : at + OWNED]
        mate_copies[p].start()

    def pair_sum(k, cols):
        p, k = k // 2, k % 2
        return prod[p, c, k, :, cols].astype(F32) + pair[p, k, :, cols].astype(F32)

    every = pl.ds(0, qlocal)
    halves = [pl.ds(h * half, half) for h in range(2)]
    a_right = remote(quads.at[0], a_in.at[0], as_sem.at[0], ar_sem.at[0], right)
    a_left = remote(quads.at[1], a_in.at[1], as_sem.at[1], ar_sem.at[1], left)
    b_right = remote(quads.at[3], b_in.at[1], bs_sem.at[0], br_sem.at[0], right)
    b_left = remote(quads.at[4], b_in.at[2], bs_sem.at[1], br_sem.at[1], left)
    m_right = [
        remote(
            quads.at[2, :, cols], b_in.at[0, :, cols], bs_sem.at[2 + h], br_sem.at[2 + h], right
        )
        for h, cols in enumerate(halves)
    ]
    m_left = [
        remote(quads.at[5, :, cols], b_in.at[3, :, cols], bs_sem.at[4 + h], br_sem.at[4 + h], left)
        for h, cols in enumerate(halves)
    ]

    load_og.wait()
    multiply(0)
    multiply(1)
    mate_copies[0].wait_recv()
    quads[0] = pair_sum(0, every).astype(BF16)
    a_right.start()
    quads[1] = pair_sum(1, every).astype(BF16)
    a_left.start()
    multiply(2)
    mate_copies[1].wait_recv()
    quads[3] = pair_sum(3, every).astype(BF16)
    b_right.start()
    mate_copies[2].wait_recv()
    quads[4] = pair_sum(4, every).astype(BF16)
    b_left.start()

    near_copies = [
        remote(parts.at[n, pl.ds(c, SENT)], recv_h.at[c, n], ns_sem.at[n], nr_sem.at[n], mate)
        for n in range(CHUNKS)
    ]
    far_copies = [
        remote(
            parts.at[n, pl.ds(1 - c, SENT)], recv_h.at[1 - c, n], fs_sem.at[n], fr_sem.at[n], far
        )
        for n in range(CHUNKS)
    ]

    def send_far(direct, first, last):
        if first < last:

            @pl.when(zl != c if direct else zl == c)
            def _():
                for n in range(first, last):
                    far_copies[n].start()

    load_cold.wait()
    for copy in cold_copies:
        copy.wait_recv()
    picked = cold_in[...].T
    for n in range(CHUNKS):
        cols = pl.ds(n * width, width)
        got = lax.dot_general(picked, og[:, cols], CONTRACT, preferred_element_type=F32)
        parts[n] = got.astype(BF16).reshape(COLD, BLOCK, width)
        if n < DIRECT[0]:
            send_far(True, n, n + 1)
    multiply(3)

    a_right.wait_recv()
    for h, cols in enumerate(halves):
        quads[2, :, cols] = (pair_sum(2, cols) + a_in[0, :, cols].astype(F32)).astype(BF16)
        m_right[h].start()
        if h == 0:
            a_left.wait_recv()
        quads[5, :, cols] = (pair_sum(5, cols) + a_in[1, :, cols].astype(F32)).astype(BF16)
        m_left[h].start()
    send_far(False, 0, DIAGONAL[0])
    for n in range(CHUNKS):
        near_copies[n].start()

    z_copies = [
        remote(z_out.at[:, cols], z_in.at[:, cols], zs_sem.at[h], zr_sem.at[h], across)
        for h, cols in enumerate(halves)
    ]
    mate_copies[3].wait_recv()
    b_right.wait_recv()
    b_left.wait_recv()
    for h, cols in enumerate(halves):
        m_right[h].wait_recv()
        m_left[h].wait_recv()
        total = b_in[1 - zl, :, cols].astype(F32) + b_in[3 - zl, :, cols].astype(F32)
        z_out[:, cols] = (pair_sum(6, cols) + total).astype(BF16)
        z_copies[h].start()
    send_far(True, DIRECT[0], DIRECT[1])
    send_far(False, DIAGONAL[0], DIAGONAL[1])
    for load in load_state:
        load.wait()

    up, down, other = tensor(1, 0), tensor(3, 0), tensor(0, 1)

    def gather(n, slot, to, h, part=None):
        if part is None:
            at = weights.at[slot, :, halves[h]]
        else:
            at = weights.at[slot, :, pl.ds(h * half + part * quarter, quarter)]
        return remote(at, at, gs_sem.at[h, n], gr_sem.at[h, n], (i, to))

    step_rows = 16

    def adam(h):
        cols = halves[h]

        def adam_step(k, carry):
            at = pl.ds(pl.multiple_of(k * step_rows, step_rows), step_rows)
            grad = prod[3, c, 1, at, cols].astype(F32) + pair[3, 1, at, cols].astype(F32)
            grad = grad + b_in[zl, at, cols].astype(F32) + b_in[2 + zl, at, cols].astype(F32)
            grad = grad + z_in[at, cols].astype(F32)
            master = state[0, at, cols]
            moment = BETA_ONE * state[1, at, cols] + (1.0 - BETA_ONE) * grad
            second = BETA_TWO * state[2, at, cols] + (1.0 - BETA_TWO) * grad * grad
            update = moment / CORRECT_ONE / (jnp.sqrt(second / CORRECT_TWO) + ADAM_EPS)
            master = master - LEARN_RATE * (update + DECAY * master)
            state[0, at, cols] = master
            state[1, at, cols] = moment
            state[2, at, cols] = second
            weights[t, at, cols] = master.astype(BF16)
            return carry

        lax.fori_loop(0, OWNED // step_rows, adam_step, 0)

    g_up, g_down, g_other = [], [], []
    for h in range(2):
        z_copies[h].wait_recv()
        adam(h)
        g_up.append(gather(0, t, up, h))
        g_down.append(gather(1, t, down, h))
        g_other.append(gather(2, t, other, h))
        g_other[h].start()
        g_up[h].start()
        g_down[h].start()
    send_far(True, DIRECT[1], DIRECT[2])
    send_far(False, DIAGONAL[1], DIAGONAL[2])

    outs = [
        pltpu.make_async_copy(state.at[k], ref, out_sem.at[k])
        for k, ref in enumerate((oma_h, omo_h, ose_h))
    ]
    for out in outs:
        out.start()

    last = []
    for h in range(2):
        g_up[h].wait_recv()
        last.append(gather(3, down, up, h, 0))
        last[-1].start()
        g_down[h].wait_recv()
        last.append(gather(4, up, down, h, 1))
        last[-1].start()
    o_up, o_down = [], []
    for h in range(2):
        g_other[h].wait_recv()
        o_up.append(gather(5, other, up, h))
        o_up[h].start()
        o_down.append(gather(6, other, down, h))
        o_down[h].start()
    for h in range(2):
        o_up[h].wait_recv()
        last.append(gather(7, tensor(3, 1), up, h, 0))
        last[-1].start()
        o_down[h].wait_recv()
        last.append(gather(8, tensor(1, 1), down, h, 1))
        last[-1].start()
    for copy in last:
        copy.wait_recv()
    out = pltpu.make_async_copy(weights, ohw_h, out_sem.at[3])
    out.start()
    outs.append(out)
    for copy in near_copies + far_copies:
        copy.wait_recv()
    for copy in started:
        copy.wait_send()
    for out in outs:
        out.wait()


def finish(own, ma, mo, se, hw, recv, oma_h, omo_h, ose_h, ohw_h, ocold_h, stage, out_sem, cold_sem):
    i = lax.axis_index("dp")
    width = recv.shape[-1]
    qlocal = width * CHUNKS
    outs = []

    def put(src, dst, sem):
        outs.append(pltpu.make_async_copy(src, dst, sem))
        outs[-1].start()

    for k, (src, dst) in enumerate(((ma, oma_h), (mo, omo_h), (se, ose_h))):
        put(src, dst, out_sem.at[k])
    for slot in range(8):
        put(hw.at[slot], ohw_h.at[:, pl.ds(slot * qlocal, qlocal)], out_sem.at[3 + slot])
    ones_prev, place_prev = slots(own, lax.rem(i + 15, 16))
    ones_next, place_next = slots(own, lax.rem(i + 1, 16))
    for n in range(CHUNKS):
        for k in range(COLD):
            a = recv[0, n, jnp.minimum(place_prev[k], SENT - 1)].astype(F32)
            b = recv[1, n, jnp.maximum(place_next[k] - 1, 0)].astype(F32)
            a = jnp.where(ones_prev[k] == 1, a, 0.0)
            b = jnp.where(ones_next[k] == 0, b, 0.0)
            stage[n, k * BLOCK : (k + 1) * BLOCK] = a + b
        put(stage.at[n], ocold_h.at[:, pl.ds(n * width, width)], cold_sem.at[n])
    for out in outs:
        out.wait()


def per_device(activations, out_grad, block_ids, owner_map, master, moment, second):
    rows, tokens, qlocal = activations.shape[0], out_grad.shape[0], out_grad.shape[1]
    width = qlocal // CHUNKS
    partners = len(OFFSETS)
    dma, like = pltpu.SemaphoreType.DMA, jax.ShapeDtypeStruct
    anywhere = pl.BlockSpec(memory_space=pl.ANY)
    hbm = pl.BlockSpec(memory_space=pltpu.HBM)
    smem = pl.BlockSpec(memory_space=pltpu.SMEM)
    vmem = pl.BlockSpec(memory_space=pltpu.VMEM)
    owners = owner_map.T
    chosen = pl.pallas_call(
        pick,
        name="pick",
        out_shape=(like((PARTS, 8, rows, 2 * BLOCK), BF16), like((8, rows, COLD * BLOCK), BF16)),
        in_specs=[smem, smem, hbm],
        out_specs=(vmem, vmem),
        scratch_shapes=[pltpu.VMEM((rows, D), BF16), dma],
        compiler_params=pltpu.CompilerParams(vmem_limit_bytes=16 * 1024 * 1024),
    )(block_ids, owners, activations)
    states = (like(master.shape, F32),) * 3
    gathered = pl.pallas_call(
        exchange,
        name="exchange",
        out_shape=(
            *states,
            like((8, OWNED, qlocal), BF16),
            like((2, CHUNKS, SENT, BLOCK, width), BF16),
        ),
        in_specs=[anywhere] * 2 + [hbm] * 4,
        out_specs=(anywhere,) * 5,
        scratch_shapes=[
            pltpu.VMEM((tokens, qlocal), BF16),
            pltpu.VMEM((3, OWNED, qlocal), F32),
            pltpu.VMEM((PARTS, tokens, 2 * BLOCK), BF16),
            pltpu.VMEM((tokens, COLD * BLOCK), BF16),
            pltpu.VMEM((PARTS, 2, 2, OWNED, qlocal), BF16),
            pltpu.VMEM((PARTS, 2, OWNED, qlocal), BF16),
            pltpu.VMEM((6, OWNED, qlocal), BF16),
            pltpu.VMEM((2, OWNED, qlocal), BF16),
            pltpu.VMEM((4, OWNED, qlocal), BF16),
            pltpu.VMEM((OWNED, qlocal), BF16),
            pltpu.VMEM((OWNED, qlocal), BF16),
            pltpu.VMEM((8, OWNED, qlocal), BF16),
            pltpu.VMEM((CHUNKS, COLD, BLOCK, width), BF16),
            dma((9,)),
            dma((4,)),
            *[dma((PARTS, partners))] * 2,
            *[dma((partners,))] * 2,
            *[dma((PARTS,))] * 2,
            *[dma((2,))] * 2,
            *[dma((6,))] * 2,
            *[dma((2,))] * 2,
            *[dma((CHUNKS,))] * 4,
            *[dma((2, 9))] * 2,
        ],
        compiler_params=pltpu.CompilerParams(
            collective_id=0, has_side_effects=True, vmem_limit_bytes=40 * 1024 * 1024
        ),
    )(*chosen, out_grad, master, moment, second)
    return pl.pallas_call(
        finish,
        name="finish",
        out_shape=(
            *states,
            like((OWNED, 8 * qlocal), BF16),
            like((COLD * BLOCK, qlocal), F32),
        ),
        in_specs=[smem] + [vmem] * 5,
        out_specs=(anywhere,) * 5,
        scratch_shapes=[
            pltpu.VMEM((CHUNKS, COLD * BLOCK, width), F32),
            dma((11,)),
            dma((CHUNKS,)),
        ],
        compiler_params=pltpu.CompilerParams(vmem_limit_bytes=24 * 1024 * 1024),
    )(owners, *gathered)


def solution(mesh):
    return jax.shard_map(
        per_device,
        mesh=mesh,
        in_specs=(
            P(("dp", "tensor"), None),
            P("dp", "tensor"),
            P(),
            P(),
            P("dp", "tensor"),
            P("dp", "tensor"),
            P("dp", "tensor"),
        ),
        out_specs=(
            P("dp", "tensor"),
            P("dp", "tensor"),
            P("dp", "tensor"),
            P("dp", None),
            P("dp", "tensor"),
        ),
        check_vma=False,
    )
```

```python
import jax
import jax.numpy as jnp
from jax import lax
from jax.experimental import pallas as pl
from jax.experimental.pallas import tpu as pltpu
from jax.sharding import PartitionSpec as P

D = 16384
BLOCK = 128
HOT = 8
COLD = 4
SENT = 3
OWNED = 64
PARTS = 4
CHUNKS = 8
DIRECT = (7, 7, 8, 8, 8, 8)
RELAYED = (0, 0, 1, 4, 7, 8)

BETA_ONE = 0.9
BETA_TWO = 0.95
ADAM_EPS = 1e-08
LEARN_RATE = 0.01
DECAY = 0.1
CORRECT_ONE = 1.0 - 0.9**10
CORRECT_TWO = 1.0 - 0.95**10

OFFSETS = ((2, 1), (1, 1), (3, 1), (0, 1), (2, 0), (1, 0), (3, 0))
CONTRACT = (((1,), (0,)), ((), ()))
F32 = jnp.float32
BF16 = jnp.bfloat16


def place(i):
    return lax.div(i, 4), lax.rem(lax.div(i, 2), 2), lax.rem(i, 2)


def hot_block(k, x, zl):
    step = (2, 2, 1, 1, 3, 3, 0, 0)[k]
    side = (0, 1, 0, 1, 0, 1, 1 - zl, zl)[k]
    return lax.rem(x + step, 4) * 2 + side


def slots(own, index):
    ones = [own[k, index] for k in range(COLD)]
    seen, places = jnp.int32(0), []
    for k in range(COLD):
        places.append(seen)
        seen = seen + ones[k]
    places = [jnp.where(ones[k] == 1, places[k], seen + k - places[k]) for k in range(COLD)]
    return ones, places


def pick(ids, own, act_h, hot, cold, act, sem):
    load = pltpu.make_async_copy(act_h, act, sem)
    load.start()
    i = lax.axis_index("dp")
    x, zl, _ = place(i)
    _, mine = slots(own, i)
    load.wait()

    def columns(block):
        return act[:, pl.ds(pl.multiple_of(block * BLOCK, BLOCK), BLOCK)]

    def group_step(group, carry):
        for k in range(HOT):
            at = k % 2 * BLOCK
            hot[k // 2, group, :, at : at + BLOCK] = columns(ids[group, hot_block(k, x, zl)])
        for slot in range(COLD):
            block = jnp.int32(0)
            for k in range(COLD):
                block = block + jnp.where(mine[k] == slot, ids[group, HOT + k], 0)
            cold[group, :, slot * BLOCK : (slot + 1) * BLOCK] = columns(block)
        return carry

    lax.fori_loop(0, cold.shape[0], group_step, 0)


def exchange(
    send_hot, send_cold, og_h, ma_h, mo_h, se_h,
    oma_h, omo_h, ose_h, ohw_h, recv_h,
    og, state, hot_in, cold_in, prod, pair, quads, a_in, b_in, z_out, z_in, weights, parts, relay,
    load_sem, out_sem, hs_sem, hr_sem, cs_sem, cr_sem, ds_sem, dr_sem, as_sem, ar_sem,
    bs_sem, br_sem, zs_sem, zr_sem, ns_sem, nr_sem, fs_sem, fr_sem, xs_sem, xr_sem,
    gs_sem, gr_sem,
):
    rows, qlocal = send_hot.shape[2], og.shape[1]
    width, half, quarter = qlocal // CHUNKS, qlocal // 2, qlocal // 4
    i = lax.axis_index("dp")
    t = lax.axis_index("tensor")
    x, zl, c = place(i)
    y, zh = lax.div(t, 2), lax.rem(t, 2)

    def device(x_, zl_, c_):
        return ((x_ * 2 + zl_) * 2 + c_, t)

    def tensor(dy, dz):
        return lax.rem(y + dy, 4) * 2 + lax.rem(zh + dz, 2)

    right, left = device(lax.rem(x + 1, 4), zl, c), device(lax.rem(x + 3, 4), zl, c)
    mate, across = device(x, zl, 1 - c), device(x, 1 - zl, c)
    corner = device(x, 1 - zl, 1 - c)

    started = []

    def remote(src, dst, send, recv, to):
        copy = pltpu.make_async_remote_copy(
            src_ref=src, dst_ref=dst, send_sem=send, recv_sem=recv, device_id=to,
            device_id_type=pl.DeviceIdType.MESH,
        )
        started.append(copy)
        return copy

    own_rows = pl.ds(pl.multiple_of(t * rows, rows), rows)
    load_og = pltpu.make_async_copy(og_h, og, load_sem.at[0])
    load_own = [
        pltpu.make_async_copy(send_hot.at[p, t], hot_in.at[p, own_rows], load_sem.at[1 + p])
        for p in range(PARTS)
    ]
    load_cold = pltpu.make_async_copy(send_cold.at[t], cold_in.at[own_rows], load_sem.at[5])
    load_state = [
        pltpu.make_async_copy(ref, state.at[k], load_sem.at[6 + k])
        for k, ref in enumerate((ma_h, mo_h, se_h))
    ]
    for load in (load_og, *load_own, load_cold, *load_state):
        load.start()

    barrier = pltpu.get_barrier_semaphore()
    peers = [(i, tensor(dy, dz)) for dy, dz in OFFSETS] + [right, left, mate, across, corner]
    for peer in peers:
        pl.semaphore_signal(barrier, inc=1, device_id=peer, device_id_type=pl.DeviceIdType.MESH)
    pl.semaphore_wait(barrier, len(peers))

    hot_copies, cold_copies = [[] for _ in range(PARTS)], []
    for p in (0, 1, 2, None, 3):
        for n, offset in enumerate(OFFSETS):
            to = tensor(*offset)
            if p is None:
                src, dst = send_cold.at[to], cold_in.at[own_rows]
                copy = remote(src, dst, cs_sem.at[n], cr_sem.at[n], (i, to))
                cold_copies.append(copy)
            else:
                src, dst = send_hot.at[p, to], hot_in.at[p, own_rows]
                copy = remote(src, dst, hs_sem.at[p, n], hr_sem.at[p, n], (i, to))
                hot_copies[p].append(copy)
            copy.start()

    mate_copies = [
        remote(prod.at[p, 1 - c], pair.at[p], ds_sem.at[p], dr_sem.at[p], mate)
        for p in range(PARTS)
    ]

    def multiply(p):
        load_own[p].wait()
        for copy in hot_copies[p]:
            copy.wait_recv()
        picked = hot_in[p].T
        for n in range(4):
            cols = pl.ds(n * quarter, quarter)
            got = lax.dot_general(picked, og[:, cols], CONTRACT, preferred_element_type=F32)
            got = got.astype(BF16)
            for k in range(2):
                for core in range(2):
                    at = k * BLOCK + core * OWNED
                    prod[p, core, k, :, cols] = got[at : at + OWNED]
        mate_copies[p].start()

    def pair_sum(k, cols):
        p, k = k // 2, k % 2
        return prod[p, c, k, :, cols].astype(F32) + pair[p, k, :, cols].astype(F32)

    every = pl.ds(0, qlocal)
    halves = [pl.ds(h * half, half) for h in range(2)]
    a_right = remote(quads.at[0], a_in.at[0], as_sem.at[0], ar_sem.at[0], right)
    a_left = remote(quads.at[1], a_in.at[1], as_sem.at[1], ar_sem.at[1], left)
    b_right = remote(quads.at[3], b_in.at[1], bs_sem.at[0], br_sem.at[0], right)
    b_left = remote(quads.at[4], b_in.at[2], bs_sem.at[1], br_sem.at[1], left)
    m_right = [
        remote(
            quads.at[2, :, cols], b_in.at[0, :, cols], bs_sem.at[2 + h], br_sem.at[2 + h], right
        )
        for h, cols in enumerate(halves)
    ]
    m_left = [
        remote(quads.at[5, :, cols], b_in.at[3, :, cols], bs_sem.at[4 + h], br_sem.at[4 + h], left)
        for h, cols in enumerate(halves)
    ]

    load_og.wait()
    multiply(0)
    multiply(1)
    mate_copies[0].wait_recv()
    quads[0] = pair_sum(0, every).astype(BF16)
    a_right.start()
    quads[1] = pair_sum(1, every).astype(BF16)
    a_left.start()
    multiply(2)
    mate_copies[1].wait_recv()
    quads[3] = pair_sum(3, every).astype(BF16)
    b_right.start()
    mate_copies[2].wait_recv()
    quads[4] = pair_sum(4, every).astype(BF16)
    b_left.start()

    near_copies = [
        remote(parts.at[n, pl.ds(c, SENT)], recv_h.at[c, n], ns_sem.at[n], nr_sem.at[n], mate)
        for n in range(CHUNKS)
    ]
    far_copies = [
        remote(
            parts.at[n, pl.ds(1 - c, SENT)], recv_h.at[1 - c, n], fs_sem.at[n], fr_sem.at[n], corner
        )
        for n in range(CHUNKS)
    ]
    onward = device(lax.rem(x + 3 + 2 * c, 4), zl, c)
    hop_copies = [
        remote(parts.at[n, pl.ds(1 - c, SENT)], relay.at[n], xs_sem.at[n], xr_sem.at[n], onward)
        for n in range(CHUNKS)
    ]
    relay_copies = [
        remote(relay.at[n], recv_h.at[1 - c, n], fs_sem.at[n], fr_sem.at[n], corner)
        for n in range(CHUNKS)
    ]
    del started[-2 * CHUNKS :]

    def send_own(first, last):
        if first < last:

            @pl.when(zl != c)
            def _():
                for n in range(first, last):
                    far_copies[n].start()

    def point(k):
        send_own(DIRECT[k - 1], DIRECT[k])
        if RELAYED[k - 1] < RELAYED[k]:

            @pl.when(zl == c)
            def _():
                for n in range(RELAYED[k - 1], RELAYED[k]):
                    hop_copies[n].wait_recv()
                    relay_copies[n].start()

    load_cold.wait()
    for copy in cold_copies:
        copy.wait_recv()
    picked = cold_in[...].T
    for n in range(CHUNKS):
        cols = pl.ds(n * width, width)
        got = lax.dot_general(picked, og[:, cols], CONTRACT, preferred_element_type=F32)
        parts[n] = got.astype(BF16).reshape(COLD, BLOCK, width)
        if n < DIRECT[0]:
            send_own(n, n + 1)
    multiply(3)

    a_right.wait_recv()
    for h, cols in enumerate(halves):
        quads[2, :, cols] = (pair_sum(2, cols) + a_in[0, :, cols].astype(F32)).astype(BF16)
        m_right[h].start()
        if h == 0:
            a_left.wait_recv()
        quads[5, :, cols] = (pair_sum(5, cols) + a_in[1, :, cols].astype(F32)).astype(BF16)
        m_left[h].start()

    @pl.when(zl == c)
    def _():
        for n in range(CHUNKS):
            hop_copies[n].start()

    point(1)
    for n in range(CHUNKS):
        near_copies[n].start()

    z_copies = [
        remote(z_out.at[:, cols], z_in.at[:, cols], zs_sem.at[h], zr_sem.at[h], across)
        for h, cols in enumerate(halves)
    ]
    mate_copies[3].wait_recv()
    b_right.wait_recv()
    b_left.wait_recv()
    for h, cols in enumerate(halves):
        m_right[h].wait_recv()
        m_left[h].wait_recv()
        total = b_in[1 - zl, :, cols].astype(F32) + b_in[3 - zl, :, cols].astype(F32)
        z_out[:, cols] = (pair_sum(6, cols) + total).astype(BF16)
        z_copies[h].start()
    point(2)
    for load in load_state:
        load.wait()

    up, down, other = tensor(1, 0), tensor(3, 0), tensor(0, 1)

    def gather(n, slot, to, h, part=None):
        if part is None:
            at = weights.at[slot, :, halves[h]]
        else:
            at = weights.at[slot, :, pl.ds(h * half + part * quarter, quarter)]
        return remote(at, at, gs_sem.at[h, n], gr_sem.at[h, n], (i, to))

    step_rows = 16

    def adam(h):
        cols = halves[h]

        def adam_step(k, carry):
            at = pl.ds(pl.multiple_of(k * step_rows, step_rows), step_rows)
            grad = prod[3, c, 1, at, cols].astype(F32) + pair[3, 1, at, cols].astype(F32)
            grad = grad + b_in[zl, at, cols].astype(F32) + b_in[2 + zl, at, cols].astype(F32)
            grad = grad + z_in[at, cols].astype(F32)
            master = state[0, at, cols]
            moment = BETA_ONE * state[1, at, cols] + (1.0 - BETA_ONE) * grad
            second = BETA_TWO * state[2, at, cols] + (1.0 - BETA_TWO) * grad * grad
            update = moment / CORRECT_ONE / (jnp.sqrt(second / CORRECT_TWO) + ADAM_EPS)
            master = master - LEARN_RATE * (update + DECAY * master)
            state[0, at, cols] = master
            state[1, at, cols] = moment
            state[2, at, cols] = second
            weights[t, at, cols] = master.astype(BF16)
            return carry

        lax.fori_loop(0, OWNED // step_rows, adam_step, 0)

    g_up, g_down, g_other = [], [], []
    for h in range(2):
        z_copies[h].wait_recv()
        adam(h)
        g_up.append(gather(0, t, up, h))
        g_down.append(gather(1, t, down, h))
        g_other.append(gather(2, t, other, h))
        g_other[h].start()
        g_up[h].start()
        g_down[h].start()
    point(3)

    outs = [
        pltpu.make_async_copy(state.at[k], ref, out_sem.at[k])
        for k, ref in enumerate((oma_h, omo_h, ose_h))
    ]
    for out in outs:
        out.start()

    last = []
    for h in range(2):
        g_up[h].wait_recv()
        last.append(gather(3, down, up, h, 0))
        last[-1].start()
        g_down[h].wait_recv()
        last.append(gather(4, up, down, h, 1))
        last[-1].start()
    point(4)
    o_up, o_down = [], []
    for h in range(2):
        g_other[h].wait_recv()
        o_up.append(gather(5, other, up, h))
        o_up[h].start()
        o_down.append(gather(6, other, down, h))
        o_down[h].start()
    point(5)
    for h in range(2):
        o_up[h].wait_recv()
        last.append(gather(7, tensor(3, 1), up, h, 0))
        last[-1].start()
        o_down[h].wait_recv()
        last.append(gather(8, tensor(1, 1), down, h, 1))
        last[-1].start()
    for copy in last:
        copy.wait_recv()
    out = pltpu.make_async_copy(weights, ohw_h, out_sem.at[3])
    out.start()
    outs.append(out)
    for copy in near_copies + far_copies:
        copy.wait_recv()
    for copy in started:
        copy.wait_send()

    @pl.when(zl == c)
    def _():
        for copy in hop_copies:
            copy.wait_send()

    for out in outs:
        out.wait()


def finish(own, ma, mo, se, hw, recv, oma_h, omo_h, ose_h, ohw_h, ocold_h, stage, out_sem, cold_sem):
    i = lax.axis_index("dp")
    width = recv.shape[-1]
    qlocal = width * CHUNKS
    outs = []

    def put(src, dst, sem):
        outs.append(pltpu.make_async_copy(src, dst, sem))
        outs[-1].start()

    for k, (src, dst) in enumerate(((ma, oma_h), (mo, omo_h), (se, ose_h))):
        put(src, dst, out_sem.at[k])
    for slot in range(8):
        put(hw.at[slot], ohw_h.at[:, pl.ds(slot * qlocal, qlocal)], out_sem.at[3 + slot])
    ones_prev, place_prev = slots(own, lax.rem(i + 15, 16))
    ones_next, place_next = slots(own, lax.rem(i + 1, 16))
    for n in range(CHUNKS):
        for k in range(COLD):
            a = recv[0, n, jnp.minimum(place_prev[k], SENT - 1)].astype(F32)
            b = recv[1, n, jnp.maximum(place_next[k] - 1, 0)].astype(F32)
            a = jnp.where(ones_prev[k] == 1, a, 0.0)
            b = jnp.where(ones_next[k] == 0, b, 0.0)
            stage[n, k * BLOCK : (k + 1) * BLOCK] = a + b
        put(stage.at[n], ocold_h.at[:, pl.ds(n * width, width)], cold_sem.at[n])
    for out in outs:
        out.wait()


def per_device(activations, out_grad, block_ids, owner_map, master, moment, second):
    rows, tokens, qlocal = activations.shape[0], out_grad.shape[0], out_grad.shape[1]
    width = qlocal // CHUNKS
    partners = len(OFFSETS)
    dma, like = pltpu.SemaphoreType.DMA, jax.ShapeDtypeStruct
    anywhere = pl.BlockSpec(memory_space=pl.ANY)
    hbm = pl.BlockSpec(memory_space=pltpu.HBM)
    smem = pl.BlockSpec(memory_space=pltpu.SMEM)
    vmem = pl.BlockSpec(memory_space=pltpu.VMEM)
    owners = owner_map.T
    chosen = pl.pallas_call(
        pick,
        name="pick",
        out_shape=(like((PARTS, 8, rows, 2 * BLOCK), BF16), like((8, rows, COLD * BLOCK), BF16)),
        in_specs=[smem, smem, hbm],
        out_specs=(vmem, vmem),
        scratch_shapes=[pltpu.VMEM((rows, D), BF16), dma],
        cost_estimate=pl.CostEstimate(flops=2000000000, bytes_accessed=3000000, transcendentals=0),
        compiler_params=pltpu.CompilerParams(vmem_limit_bytes=16 * 1024 * 1024),
    )(block_ids, owners, activations)
    states = (like(master.shape, F32),) * 3
    gathered = pl.pallas_call(
        exchange,
        name="exchange",
        out_shape=(
            *states,
            like((8, OWNED, qlocal), BF16),
            like((2, CHUNKS, SENT, BLOCK, width), BF16),
        ),
        in_specs=[anywhere] * 2 + [hbm] * 4,
        out_specs=(anywhere,) * 5,
        scratch_shapes=[
            pltpu.VMEM((tokens, qlocal), BF16),
            pltpu.VMEM((3, OWNED, qlocal), F32),
            pltpu.VMEM((PARTS, tokens, 2 * BLOCK), BF16),
            pltpu.VMEM((tokens, COLD * BLOCK), BF16),
            pltpu.VMEM((PARTS, 2, 2, OWNED, qlocal), BF16),
            pltpu.VMEM((PARTS, 2, OWNED, qlocal), BF16),
            pltpu.VMEM((6, OWNED, qlocal), BF16),
            pltpu.VMEM((2, OWNED, qlocal), BF16),
            pltpu.VMEM((4, OWNED, qlocal), BF16),
            pltpu.VMEM((OWNED, qlocal), BF16),
            pltpu.VMEM((OWNED, qlocal), BF16),
            pltpu.VMEM((8, OWNED, qlocal), BF16),
            pltpu.VMEM((CHUNKS, COLD, BLOCK, width), BF16),
            pltpu.VMEM((CHUNKS, SENT, BLOCK, width), BF16),
            dma((9,)),
            dma((4,)),
            *[dma((PARTS, partners))] * 2,
            *[dma((partners,))] * 2,
            *[dma((PARTS,))] * 2,
            *[dma((2,))] * 2,
            *[dma((6,))] * 2,
            *[dma((2,))] * 2,
            *[dma((CHUNKS,))] * 6,
            *[dma((2, 9))] * 2,
        ],
        compiler_params=pltpu.CompilerParams(
            collective_id=0, has_side_effects=True, vmem_limit_bytes=40 * 1024 * 1024
        ),
    )(*chosen, out_grad, master, moment, second)
    return pl.pallas_call(
        finish,
        name="finish",
        out_shape=(
            *states,
            like((OWNED, 8 * qlocal), BF16),
            like((COLD * BLOCK, qlocal), F32),
        ),
        in_specs=[smem] + [vmem] * 5,
        out_specs=(anywhere,) * 5,
        scratch_shapes=[
            pltpu.VMEM((CHUNKS, COLD * BLOCK, width), F32),
            dma((11,)),
            dma((CHUNKS,)),
        ],
        compiler_params=pltpu.CompilerParams(vmem_limit_bytes=24 * 1024 * 1024),
    )(owners, *gathered)


def solution(mesh):
    return jax.shard_map(
        per_device,
        mesh=mesh,
        in_specs=(
            P(("dp", "tensor"), None),
            P("dp", "tensor"),
            P(),
            P(),
            P("dp", "tensor"),
            P("dp", "tensor"),
            P("dp", "tensor"),
        ),
        out_specs=(
            P("dp", "tensor"),
            P("dp", "tensor"),
            P("dp", "tensor"),
            P("dp", None),
            P("dp", "tensor"),
        ),
        check_vma=False,
    )
```

```python
import jax
import jax.numpy as jnp
from jax import lax
from jax.experimental import pallas as pl
from jax.experimental.pallas import tpu as pltpu
from jax.sharding import PartitionSpec as P

D = 16384
BLOCK = 128
HOT = 8
COLD = 4
SENT = 3
OWNED = 64
PARTS = 4
ORDER = (0, 1, None, 2, 3)
CHUNKS = 8
DIRECT = (0, 0, 2, 8, 8, 8, 8)
DIAGONAL = (8, 8, 8, 8, 8, 8, 8)
RELAYED = (0, 4, 6, 8, 8, 8, 8)

BETA_ONE = 0.9
BETA_TWO = 0.95
ADAM_EPS = 1e-08
LEARN_RATE = 0.01
DECAY = 0.1
CORRECT_ONE = 1.0 - 0.9**10
CORRECT_TWO = 1.0 - 0.95**10

OFFSETS = ((2, 1), (1, 1), (3, 1), (0, 1), (2, 0), (1, 0), (3, 0))
CONTRACT = (((1,), (0,)), ((), ()))
F32 = jnp.float32
BF16 = jnp.bfloat16


def place(i):
    return lax.div(i, 4), lax.rem(lax.div(i, 2), 2), lax.rem(i, 2)


def hot_block(k, x, zl):
    step = (2, 2, 1, 1, 3, 3, 0, 0)[k]
    side = (0, 1, 0, 1, 0, 1, 1 - zl, zl)[k]
    return lax.rem(x + step, 4) * 2 + side


def slots(own, index):
    ones = [own[k, index] for k in range(COLD)]
    seen, places = jnp.int32(0), []
    for k in range(COLD):
        places.append(seen)
        seen = seen + ones[k]
    places = [jnp.where(ones[k] == 1, places[k], seen + k - places[k]) for k in range(COLD)]
    return ones, places


def pick(ids, own, act_h, hot, cold, act, sem):
    load = pltpu.make_async_copy(act_h, act, sem)
    load.start()
    i = lax.axis_index("dp")
    x, zl, _ = place(i)
    _, mine = slots(own, i)
    load.wait()

    def columns(block):
        return act[:, pl.ds(pl.multiple_of(block * BLOCK, BLOCK), BLOCK)]

    def group_step(group, carry):
        for k in range(HOT):
            at = k % 2 * BLOCK
            hot[k // 2, group, :, at : at + BLOCK] = columns(ids[group, hot_block(k, x, zl)])
        for slot in range(COLD):
            block = jnp.int32(0)
            for k in range(COLD):
                block = block + jnp.where(mine[k] == slot, ids[group, HOT + k], 0)
            cold[group, :, slot * BLOCK : (slot + 1) * BLOCK] = columns(block)
        return carry

    lax.fori_loop(0, cold.shape[0], group_step, 0)


def exchange(
    send_hot, send_cold, og_h, ma_h, mo_h, se_h,
    oma_h, omo_h, ose_h, ohw_h, recv_h,
    og, state, hot_in, cold_in, prod, pair, quads, a_in, b_in, z_out, z_in, weights, parts, relay,
    load_sem, out_sem, hs_sem, hr_sem, cs_sem, cr_sem, ds_sem, dr_sem, as_sem, ar_sem,
    bs_sem, br_sem, zs_sem, zr_sem, ns_sem, nr_sem, fs_sem, fr_sem, xs_sem, xr_sem,
    gs_sem, gr_sem,
):
    rows, qlocal = send_hot.shape[2], og.shape[1]
    width, half, quarter = qlocal // CHUNKS, qlocal // 2, qlocal // 4
    i = lax.axis_index("dp")
    t = lax.axis_index("tensor")
    x, zl, c = place(i)
    y, zh = lax.div(t, 2), lax.rem(t, 2)

    def device(x_, zl_, c_):
        return ((x_ * 2 + zl_) * 2 + c_, t)

    def tensor(dy, dz):
        return lax.rem(y + dy, 4) * 2 + lax.rem(zh + dz, 2)

    right, left = device(lax.rem(x + 1, 4), zl, c), device(lax.rem(x + 3, 4), zl, c)
    mate, across = device(x, zl, 1 - c), device(x, 1 - zl, c)
    corner = device(x, 1 - zl, 1 - c)

    started = []

    def remote(src, dst, send, recv, to):
        copy = pltpu.make_async_remote_copy(
            src_ref=src, dst_ref=dst, send_sem=send, recv_sem=recv, device_id=to,
            device_id_type=pl.DeviceIdType.MESH,
        )
        started.append(copy)
        return copy

    own_rows = pl.ds(pl.multiple_of(t * rows, rows), rows)
    load_og = pltpu.make_async_copy(og_h, og, load_sem.at[0])
    load_own = [
        pltpu.make_async_copy(send_hot.at[p, t], hot_in.at[p, own_rows], load_sem.at[1 + p])
        for p in range(PARTS)
    ]
    load_cold = pltpu.make_async_copy(send_cold.at[t], cold_in.at[own_rows], load_sem.at[5])
    load_state = [
        pltpu.make_async_copy(ref, state.at[k], load_sem.at[6 + k])
        for k, ref in enumerate((ma_h, mo_h, se_h))
    ]
    for load in (load_og, *load_own, load_cold, *load_state):
        load.start()

    barrier = pltpu.get_barrier_semaphore()
    peers = [(i, tensor(dy, dz)) for dy, dz in OFFSETS] + [right, left, mate, across, corner]
    for peer in peers:
        pl.semaphore_signal(barrier, inc=1, device_id=peer, device_id_type=pl.DeviceIdType.MESH)
    pl.semaphore_wait(barrier, len(peers))

    hot_copies, cold_copies = [[] for _ in range(PARTS)], []
    for p in ORDER:
        for n, offset in enumerate(OFFSETS):
            to = tensor(*offset)
            if p is None:
                src, dst = send_cold.at[to], cold_in.at[own_rows]
                copy = remote(src, dst, cs_sem.at[n], cr_sem.at[n], (i, to))
                cold_copies.append(copy)
            else:
                src, dst = send_hot.at[p, to], hot_in.at[p, own_rows]
                copy = remote(src, dst, hs_sem.at[p, n], hr_sem.at[p, n], (i, to))
                hot_copies[p].append(copy)
            copy.start()

    mate_copies = [
        remote(prod.at[p, 1 - c], pair.at[p], ds_sem.at[p], dr_sem.at[p], mate)
        for p in range(PARTS)
    ]

    def multiply(p):
        load_own[p].wait()
        for copy in hot_copies[p]:
            copy.wait_recv()
        picked = hot_in[p].T
        for n in range(4):
            cols = pl.ds(n * quarter, quarter)
            got = lax.dot_general(picked, og[:, cols], CONTRACT, preferred_element_type=F32)
            got = got.astype(BF16)
            for k in range(2):
                for core in range(2):
                    at = k * BLOCK + core * OWNED
                    prod[p, core, k, :, cols] = got[at : at + OWNED]
        mate_copies[p].start()

    def pair_sum(k, cols):
        p, k = k // 2, k % 2
        return prod[p, c, k, :, cols].astype(F32) + pair[p, k, :, cols].astype(F32)

    every = pl.ds(0, qlocal)
    halves = [pl.ds(h * half, half) for h in range(2)]
    a_right = remote(quads.at[0], a_in.at[0], as_sem.at[0], ar_sem.at[0], right)
    a_left = remote(quads.at[1], a_in.at[1], as_sem.at[1], ar_sem.at[1], left)
    b_right = remote(quads.at[3], b_in.at[1], bs_sem.at[0], br_sem.at[0], right)
    b_left = remote(quads.at[4], b_in.at[2], bs_sem.at[1], br_sem.at[1], left)
    m_right = [
        remote(
            quads.at[2, :, cols], b_in.at[0, :, cols], bs_sem.at[2 + h], br_sem.at[2 + h], right
        )
        for h, cols in enumerate(halves)
    ]
    m_left = [
        remote(quads.at[5, :, cols], b_in.at[3, :, cols], bs_sem.at[4 + h], br_sem.at[4 + h], left)
        for h, cols in enumerate(halves)
    ]

    near_copies = [
        remote(parts.at[n, pl.ds(c, SENT)], recv_h.at[c, n], ns_sem.at[n], nr_sem.at[n], mate)
        for n in range(CHUNKS)
    ]
    far_copies = [
        remote(
            parts.at[n, pl.ds(1 - c, SENT)], recv_h.at[1 - c, n], fs_sem.at[n], fr_sem.at[n], corner
        )
        for n in range(CHUNKS)
    ]
    lift_copies = [
        remote(parts.at[n, pl.ds(1 - c, SENT)], relay.at[n], fs_sem.at[n], fr_sem.at[n], corner)
        for n in range(CHUNKS)
    ]
    onward = device(lax.rem(x + 1 + 2 * c, 4), zl, c)
    relay_copies = [
        remote(relay.at[n], recv_h.at[c, n], xs_sem.at[n], xr_sem.at[n], onward)
        for n in range(CHUNKS)
    ]
    del started[-2 * CHUNKS :]

    def send_far(direct, first, last):
        if first < last:

            @pl.when(zl != c if direct else zl == c)
            def _():
                for n in range(first, last):
                    (far_copies if direct else lift_copies)[n].start()

    def point(k):
        if RELAYED[k - 1] < RELAYED[k]:

            @pl.when(zl == c)
            def _():
                for n in range(RELAYED[k - 1], RELAYED[k]):
                    lift_copies[n].wait_recv()
                    relay_copies[n].start()

        send_far(True, DIRECT[k - 1], DIRECT[k])
        send_far(False, DIAGONAL[k - 1], DIAGONAL[k])

    def cold_products():
        load_cold.wait()
        for copy in cold_copies:
            copy.wait_recv()
        picked = cold_in[...].T
        for n in range(CHUNKS):
            cols = pl.ds(n * width, width)
            got = lax.dot_general(picked, og[:, cols], CONTRACT, preferred_element_type=F32)
            parts[n] = got.astype(BF16).reshape(COLD, BLOCK, width)
            if n < DIRECT[0]:
                send_far(True, n, n + 1)
            if n < DIAGONAL[0]:
                send_far(False, n, n + 1)

    load_og.wait()
    multiply(0)
    multiply(1)
    mate_copies[0].wait_recv()
    quads[0] = pair_sum(0, every).astype(BF16)
    a_right.start()
    quads[1] = pair_sum(1, every).astype(BF16)
    a_left.start()
    cold_products()
    multiply(2)
    mate_copies[1].wait_recv()
    quads[3] = pair_sum(3, every).astype(BF16)
    b_right.start()
    mate_copies[2].wait_recv()
    quads[4] = pair_sum(4, every).astype(BF16)
    b_left.start()
    multiply(3)

    a_right.wait_recv()
    for h, cols in enumerate(halves):
        quads[2, :, cols] = (pair_sum(2, cols) + a_in[0, :, cols].astype(F32)).astype(BF16)
        m_right[h].start()
        if h == 0:
            a_left.wait_recv()
        quads[5, :, cols] = (pair_sum(5, cols) + a_in[1, :, cols].astype(F32)).astype(BF16)
        m_left[h].start()
    point(1)
    for n in range(CHUNKS):
        near_copies[n].start()

    z_copies = [
        remote(z_out.at[:, cols], z_in.at[:, cols], zs_sem.at[h], zr_sem.at[h], across)
        for h, cols in enumerate(halves)
    ]
    mate_copies[3].wait_recv()
    b_right.wait_recv()
    b_left.wait_recv()
    for h, cols in enumerate(halves):
        m_right[h].wait_recv()
        m_left[h].wait_recv()
        total = b_in[1 - zl, :, cols].astype(F32) + b_in[3 - zl, :, cols].astype(F32)
        z_out[:, cols] = (pair_sum(6, cols) + total).astype(BF16)
        z_copies[h].start()
    point(2)
    for load in load_state:
        load.wait()

    up, down, other = tensor(1, 0), tensor(3, 0), tensor(0, 1)

    def gather(n, slot, to, h, part=None):
        if part is None:
            at = weights.at[slot, :, halves[h]]
        else:
            at = weights.at[slot, :, pl.ds(h * half + part * quarter, quarter)]
        return remote(at, at, gs_sem.at[h, n], gr_sem.at[h, n], (i, to))

    step_rows = 16

    def adam(h):
        cols = halves[h]

        def adam_step(k, carry):
            at = pl.ds(pl.multiple_of(k * step_rows, step_rows), step_rows)
            grad = prod[3, c, 1, at, cols].astype(F32) + pair[3, 1, at, cols].astype(F32)
            grad = grad + b_in[zl, at, cols].astype(F32) + b_in[2 + zl, at, cols].astype(F32)
            grad = grad + z_in[at, cols].astype(F32)
            master = state[0, at, cols]
            moment = BETA_ONE * state[1, at, cols] + (1.0 - BETA_ONE) * grad
            second = BETA_TWO * state[2, at, cols] + (1.0 - BETA_TWO) * grad * grad
            update = moment / CORRECT_ONE / (jnp.sqrt(second / CORRECT_TWO) + ADAM_EPS)
            master = master - LEARN_RATE * (update + DECAY * master)
            state[0, at, cols] = master
            state[1, at, cols] = moment
            state[2, at, cols] = second
            weights[t, at, cols] = master.astype(BF16)
            return carry

        lax.fori_loop(0, OWNED // step_rows, adam_step, 0)

    g_up, g_down, g_other = [], [], []
    for h in range(2):
        z_copies[h].wait_recv()
        adam(h)
        g_up.append(gather(0, t, up, h))
        g_down.append(gather(1, t, down, h))
        g_other.append(gather(2, t, other, h))
        g_other[h].start()
        g_up[h].start()
        g_down[h].start()
    point(3)

    outs = [
        pltpu.make_async_copy(state.at[k], ref, out_sem.at[k])
        for k, ref in enumerate((oma_h, omo_h, ose_h))
    ]
    for out in outs:
        out.start()

    last = []
    for h in range(2):
        g_up[h].wait_recv()
        last.append(gather(3, down, up, h, 0))
        last[-1].start()
        g_down[h].wait_recv()
        last.append(gather(4, up, down, h, 1))
        last[-1].start()
    point(4)
    o_up, o_down = [], []
    for h in range(2):
        g_other[h].wait_recv()
        o_up.append(gather(5, other, up, h))
        o_up[h].start()
        o_down.append(gather(6, other, down, h))
        o_down[h].start()
    point(5)
    for h in range(2):
        o_up[h].wait_recv()
        last.append(gather(7, tensor(3, 1), up, h, 0))
        last[-1].start()
        o_down[h].wait_recv()
        last.append(gather(8, tensor(1, 1), down, h, 1))
        last[-1].start()
    for copy in last:
        copy.wait_recv()
    out = pltpu.make_async_copy(weights, ohw_h, out_sem.at[3])
    out.start()
    outs.append(out)
    point(6)
    for copy in near_copies:
        copy.wait_recv()

    @pl.when(zl != c)
    def _():
        for copy in far_copies:
            copy.wait_recv()

    @pl.when(zl == c)
    def _():
        for copy in relay_copies:
            copy.wait_recv()
            copy.wait_send()

    for copy in started:
        copy.wait_send()
    for out in outs:
        out.wait()


def finish(own, ma, mo, se, hw, recv, oma_h, omo_h, ose_h, ohw_h, ocold_h, stage, out_sem, cold_sem):
    i = lax.axis_index("dp")
    width = recv.shape[-1]
    qlocal = width * CHUNKS
    outs = []

    def put(src, dst, sem):
        outs.append(pltpu.make_async_copy(src, dst, sem))
        outs[-1].start()

    for k, (src, dst) in enumerate(((ma, oma_h), (mo, omo_h), (se, ose_h))):
        put(src, dst, out_sem.at[k])
    for slot in range(8):
        put(hw.at[slot], ohw_h.at[:, pl.ds(slot * qlocal, qlocal)], out_sem.at[3 + slot])
    ones_prev, place_prev = slots(own, lax.rem(i + 15, 16))
    ones_next, place_next = slots(own, lax.rem(i + 1, 16))
    for n in range(CHUNKS):
        for k in range(COLD):
            a = recv[0, n, jnp.minimum(place_prev[k], SENT - 1)].astype(F32)
            b = recv[1, n, jnp.maximum(place_next[k] - 1, 0)].astype(F32)
            a = jnp.where(ones_prev[k] == 1, a, 0.0)
            b = jnp.where(ones_next[k] == 0, b, 0.0)
            stage[n, k * BLOCK : (k + 1) * BLOCK] = a + b
        put(stage.at[n], ocold_h.at[:, pl.ds(n * width, width)], cold_sem.at[n])
    for out in outs:
        out.wait()


def per_device(activations, out_grad, block_ids, owner_map, master, moment, second):
    rows, tokens, qlocal = activations.shape[0], out_grad.shape[0], out_grad.shape[1]
    width = qlocal // CHUNKS
    partners = len(OFFSETS)
    dma, like = pltpu.SemaphoreType.DMA, jax.ShapeDtypeStruct
    anywhere = pl.BlockSpec(memory_space=pl.ANY)
    hbm = pl.BlockSpec(memory_space=pltpu.HBM)
    smem = pl.BlockSpec(memory_space=pltpu.SMEM)
    vmem = pl.BlockSpec(memory_space=pltpu.VMEM)
    owners = owner_map.T
    chosen = pl.pallas_call(
        pick,
        name="pick",
        out_shape=(like((PARTS, 8, rows, 2 * BLOCK), BF16), like((8, rows, COLD * BLOCK), BF16)),
        in_specs=[smem, smem, hbm],
        out_specs=(vmem, vmem),
        scratch_shapes=[pltpu.VMEM((rows, D), BF16), dma],
        cost_estimate=pl.CostEstimate(flops=2000000000, bytes_accessed=3000000, transcendentals=0),
        compiler_params=pltpu.CompilerParams(vmem_limit_bytes=16 * 1024 * 1024),
    )(block_ids, owners, activations)
    states = (like(master.shape, F32),) * 3
    gathered = pl.pallas_call(
        exchange,
        name="exchange",
        out_shape=(
            *states,
            like((8, OWNED, qlocal), BF16),
            like((2, CHUNKS, SENT, BLOCK, width), BF16),
        ),
        in_specs=[anywhere] * 2 + [hbm] * 4,
        out_specs=(anywhere,) * 5,
        scratch_shapes=[
            pltpu.VMEM((tokens, qlocal), BF16),
            pltpu.VMEM((3, OWNED, qlocal), F32),
            pltpu.VMEM((PARTS, tokens, 2 * BLOCK), BF16),
            pltpu.VMEM((tokens, COLD * BLOCK), BF16),
            pltpu.VMEM((PARTS, 2, 2, OWNED, qlocal), BF16),
            pltpu.VMEM((PARTS, 2, OWNED, qlocal), BF16),
            pltpu.VMEM((6, OWNED, qlocal), BF16),
            pltpu.VMEM((2, OWNED, qlocal), BF16),
            pltpu.VMEM((4, OWNED, qlocal), BF16),
            pltpu.VMEM((OWNED, qlocal), BF16),
            pltpu.VMEM((OWNED, qlocal), BF16),
            pltpu.VMEM((8, OWNED, qlocal), BF16),
            pltpu.VMEM((CHUNKS, COLD, BLOCK, width), BF16),
            pltpu.VMEM((CHUNKS, SENT, BLOCK, width), BF16),
            dma((9,)),
            dma((4,)),
            *[dma((PARTS, partners))] * 2,
            *[dma((partners,))] * 2,
            *[dma((PARTS,))] * 2,
            *[dma((2,))] * 2,
            *[dma((6,))] * 2,
            *[dma((2,))] * 2,
            *[dma((CHUNKS,))] * 6,
            *[dma((2, 9))] * 2,
        ],
        compiler_params=pltpu.CompilerParams(
            collective_id=0, has_side_effects=True, vmem_limit_bytes=40 * 1024 * 1024
        ),
    )(*chosen, out_grad, master, moment, second)
    return pl.pallas_call(
        finish,
        name="finish",
        out_shape=(
            *states,
            like((OWNED, 8 * qlocal), BF16),
            like((COLD * BLOCK, qlocal), F32),
        ),
        in_specs=[smem] + [vmem] * 5,
        out_specs=(anywhere,) * 5,
        scratch_shapes=[
            pltpu.VMEM((CHUNKS, COLD * BLOCK, width), F32),
            dma((11,)),
            dma((CHUNKS,)),
        ],
        compiler_params=pltpu.CompilerParams(vmem_limit_bytes=24 * 1024 * 1024),
    )(owners, *gathered)


def solution(mesh):
    return jax.shard_map(
        per_device,
        mesh=mesh,
        in_specs=(
            P(("dp", "tensor"), None),
            P("dp", "tensor"),
            P(),
            P(),
            P("dp", "tensor"),
            P("dp", "tensor"),
            P("dp", "tensor"),
        ),
        out_specs=(
            P("dp", "tensor"),
            P("dp", "tensor"),
            P("dp", "tensor"),
            P("dp", None),
            P("dp", "tensor"),
        ),
        check_vma=False,
    )
```

```python
import jax
import jax.numpy as jnp
from jax import lax
from jax.experimental import pallas as pl
from jax.experimental.pallas import tpu as pltpu
from jax.sharding import PartitionSpec as P

D = 16384
BLOCK = 128
HOT = 8
COLD = 4
SENT = 3
OWNED = 64
PARTS = 4
ORDER = (0, 1, None, 2, 3)
CHUNKS = 8
DIRECT = (0, 0, 2, 4, 8, 8, 8)
DIAGONAL = (8, 8, 8, 8, 8, 8, 8)
RELAYED = (0, 4, 6, 8, 8, 8, 8)

BETA_ONE = 0.9
BETA_TWO = 0.95
ADAM_EPS = 1e-08
LEARN_RATE = 0.01
DECAY = 0.1
CORRECT_ONE = 1.0 - 0.9**10
CORRECT_TWO = 1.0 - 0.95**10

OFFSETS = ((2, 1), (1, 1), (3, 1), (0, 1), (2, 0), (1, 0), (3, 0))
CONTRACT = (((1,), (0,)), ((), ()))
F32 = jnp.float32
BF16 = jnp.bfloat16


def place(i):
    return lax.div(i, 4), lax.rem(lax.div(i, 2), 2), lax.rem(i, 2)


def hot_block(k, x, zl):
    step = (2, 2, 1, 1, 3, 3, 0, 0)[k]
    side = (0, 1, 0, 1, 0, 1, 1 - zl, zl)[k]
    return lax.rem(x + step, 4) * 2 + side


def slots(own, index):
    ones = [own[k, index] for k in range(COLD)]
    seen, places = jnp.int32(0), []
    for k in range(COLD):
        places.append(seen)
        seen = seen + ones[k]
    places = [jnp.where(ones[k] == 1, places[k], seen + k - places[k]) for k in range(COLD)]
    return ones, places


def pick(ids, own, act_h, hot, cold, act, sem):
    load = pltpu.make_async_copy(act_h, act, sem)
    load.start()
    i = lax.axis_index("dp")
    x, zl, _ = place(i)
    _, mine = slots(own, i)
    load.wait()

    def columns(block):
        return act[:, pl.ds(pl.multiple_of(block * BLOCK, BLOCK), BLOCK)]

    def group_step(group, carry):
        for k in range(HOT):
            at = k % 2 * BLOCK
            hot[k // 2, group, :, at : at + BLOCK] = columns(ids[group, hot_block(k, x, zl)])
        for slot in range(COLD):
            block = jnp.int32(0)
            for k in range(COLD):
                block = block + jnp.where(mine[k] == slot, ids[group, HOT + k], 0)
            cold[group, :, slot * BLOCK : (slot + 1) * BLOCK] = columns(block)
        return carry

    lax.fori_loop(0, cold.shape[0], group_step, 0)


def exchange(
    send_hot, send_cold, og_h, ma_h, mo_h, se_h,
    oma_h, omo_h, ose_h, ohw_h, recv_h,
    og, state, hot_in, cold_in, prod, pair, quads, a_in, b_in, z_out, z_in, weights, parts, relay,
    load_sem, out_sem, hs_sem, hr_sem, cs_sem, cr_sem, ds_sem, dr_sem, as_sem, ar_sem,
    bs_sem, br_sem, zs_sem, zr_sem, ns_sem, nr_sem, fs_sem, fr_sem, xs_sem, xr_sem,
    gs_sem, gr_sem,
):
    rows, qlocal = send_hot.shape[2], og.shape[1]
    width, half, quarter = qlocal // CHUNKS, qlocal // 2, qlocal // 4
    i = lax.axis_index("dp")
    t = lax.axis_index("tensor")
    x, zl, c = place(i)
    y, zh = lax.div(t, 2), lax.rem(t, 2)

    def device(x_, zl_, c_):
        return ((x_ * 2 + zl_) * 2 + c_, t)

    def tensor(dy, dz):
        return lax.rem(y + dy, 4) * 2 + lax.rem(zh + dz, 2)

    right, left = device(lax.rem(x + 1, 4), zl, c), device(lax.rem(x + 3, 4), zl, c)
    mate, across = device(x, zl, 1 - c), device(x, 1 - zl, c)
    corner = device(x, 1 - zl, 1 - c)

    started = []

    def remote(src, dst, send, recv, to):
        copy = pltpu.make_async_remote_copy(
            src_ref=src, dst_ref=dst, send_sem=send, recv_sem=recv, device_id=to,
            device_id_type=pl.DeviceIdType.MESH,
        )
        started.append(copy)
        return copy

    own_rows = pl.ds(pl.multiple_of(t * rows, rows), rows)
    load_og = pltpu.make_async_copy(og_h, og, load_sem.at[0])
    load_own = [
        pltpu.make_async_copy(send_hot.at[p, t], hot_in.at[p, own_rows], load_sem.at[1 + p])
        for p in range(PARTS)
    ]
    load_cold = pltpu.make_async_copy(send_cold.at[t], cold_in.at[own_rows], load_sem.at[5])
    load_state = [
        pltpu.make_async_copy(ref, state.at[k], load_sem.at[6 + k])
        for k, ref in enumerate((ma_h, mo_h, se_h))
    ]
    for load in (load_og, *load_own, load_cold, *load_state):
        load.start()

    barrier = pltpu.get_barrier_semaphore()
    peers = [(i, tensor(dy, dz)) for dy, dz in OFFSETS] + [right, left, mate, across, corner]
    for peer in peers:
        pl.semaphore_signal(barrier, inc=1, device_id=peer, device_id_type=pl.DeviceIdType.MESH)
    pl.semaphore_wait(barrier, len(peers))

    hot_copies, cold_copies = [[] for _ in range(PARTS)], []
    for p in ORDER:
        for n, offset in enumerate(OFFSETS):
            to = tensor(*offset)
            if p is None:
                src, dst = send_cold.at[to], cold_in.at[own_rows]
                copy = remote(src, dst, cs_sem.at[n], cr_sem.at[n], (i, to))
                cold_copies.append(copy)
            else:
                src, dst = send_hot.at[p, to], hot_in.at[p, own_rows]
                copy = remote(src, dst, hs_sem.at[p, n], hr_sem.at[p, n], (i, to))
                hot_copies[p].append(copy)
            copy.start()

    mate_copies = [
        remote(prod.at[p, 1 - c], pair.at[p], ds_sem.at[p], dr_sem.at[p], mate)
        for p in range(PARTS)
    ]

    def multiply(p):
        load_own[p].wait()
        for copy in hot_copies[p]:
            copy.wait_recv()
        picked = hot_in[p].T
        for n in range(4):
            cols = pl.ds(n * quarter, quarter)
            got = lax.dot_general(picked, og[:, cols], CONTRACT, preferred_element_type=F32)
            got = got.astype(BF16)
            for k in range(2):
                for core in range(2):
                    at = k * BLOCK + core * OWNED
                    prod[p, core, k, :, cols] = got[at : at + OWNED]
        mate_copies[p].start()

    def pair_sum(k, cols):
        p, k = k // 2, k % 2
        return prod[p, c, k, :, cols].astype(F32) + pair[p, k, :, cols].astype(F32)

    every = pl.ds(0, qlocal)
    halves = [pl.ds(h * half, half) for h in range(2)]
    a_right = remote(quads.at[0], a_in.at[0], as_sem.at[0], ar_sem.at[0], right)
    a_left = remote(quads.at[1], a_in.at[1], as_sem.at[1], ar_sem.at[1], left)
    b_right = remote(quads.at[3], b_in.at[1], bs_sem.at[0], br_sem.at[0], right)
    b_left = remote(quads.at[4], b_in.at[2], bs_sem.at[1], br_sem.at[1], left)
    m_right = [
        remote(
            quads.at[2, :, cols], b_in.at[0, :, cols], bs_sem.at[2 + h], br_sem.at[2 + h], right
        )
        for h, cols in enumerate(halves)
    ]
    m_left = [
        remote(quads.at[5, :, cols], b_in.at[3, :, cols], bs_sem.at[4 + h], br_sem.at[4 + h], left)
        for h, cols in enumerate(halves)
    ]

    near_copies = [
        remote(parts.at[n, pl.ds(c, SENT)], recv_h.at[c, n], ns_sem.at[n], nr_sem.at[n], mate)
        for n in range(CHUNKS)
    ]
    far_copies = [
        remote(
            parts.at[n, pl.ds(1 - c, SENT)], recv_h.at[1 - c, n], fs_sem.at[n], fr_sem.at[n], corner
        )
        for n in range(CHUNKS)
    ]
    lift_copies = [
        remote(parts.at[n, pl.ds(1 - c, SENT)], relay.at[n], fs_sem.at[n], fr_sem.at[n], corner)
        for n in range(CHUNKS)
    ]
    onward = device(lax.rem(x + 1 + 2 * c, 4), zl, c)
    relay_copies = [
        remote(relay.at[n], recv_h.at[c, n], xs_sem.at[n], xr_sem.at[n], onward)
        for n in range(CHUNKS)
    ]
    del started[-2 * CHUNKS :]

    def send_far(direct, first, last):
        if first < last:

            @pl.when(zl != c if direct else zl == c)
            def _():
                for n in range(first, last):
                    (far_copies if direct else lift_copies)[n].start()

    def point(k):
        if RELAYED[k - 1] < RELAYED[k]:

            @pl.when(zl == c)
            def _():
                for n in range(RELAYED[k - 1], RELAYED[k]):
                    lift_copies[n].wait_recv()
                    relay_copies[n].start()

        send_far(True, DIRECT[k - 1], DIRECT[k])
        send_far(False, DIAGONAL[k - 1], DIAGONAL[k])

    def cold_products():
        load_cold.wait()
        for copy in cold_copies:
            copy.wait_recv()
        picked = cold_in[...].T
        for n in range(CHUNKS):
            cols = pl.ds(n * width, width)
            got = lax.dot_general(picked, og[:, cols], CONTRACT, preferred_element_type=F32)
            parts[n] = got.astype(BF16).reshape(COLD, BLOCK, width)
            if n < DIRECT[0]:
                send_far(True, n, n + 1)
            if n < DIAGONAL[0]:
                send_far(False, n, n + 1)

    load_og.wait()
    multiply(0)
    multiply(1)
    mate_copies[0].wait_recv()
    quads[0] = pair_sum(0, every).astype(BF16)
    a_right.start()
    quads[1] = pair_sum(1, every).astype(BF16)
    a_left.start()
    cold_products()
    multiply(2)
    mate_copies[1].wait_recv()
    quads[3] = pair_sum(3, every).astype(BF16)
    b_right.start()
    mate_copies[2].wait_recv()
    quads[4] = pair_sum(4, every).astype(BF16)
    b_left.start()
    multiply(3)

    a_right.wait_recv()
    for h, cols in enumerate(halves):
        quads[2, :, cols] = (pair_sum(2, cols) + a_in[0, :, cols].astype(F32)).astype(BF16)
        m_right[h].start()
        if h == 0:
            a_left.wait_recv()
        quads[5, :, cols] = (pair_sum(5, cols) + a_in[1, :, cols].astype(F32)).astype(BF16)
        m_left[h].start()
    point(1)
    for n in range(CHUNKS):
        near_copies[n].start()

    z_copies = [
        remote(z_out.at[:, cols], z_in.at[:, cols], zs_sem.at[h], zr_sem.at[h], across)
        for h, cols in enumerate(halves)
    ]
    mate_copies[3].wait_recv()
    b_right.wait_recv()
    b_left.wait_recv()
    for h, cols in enumerate(halves):
        m_right[h].wait_recv()
        m_left[h].wait_recv()
        total = b_in[1 - zl, :, cols].astype(F32) + b_in[3 - zl, :, cols].astype(F32)
        z_out[:, cols] = (pair_sum(6, cols) + total).astype(BF16)
        z_copies[h].start()
    point(2)
    for load in load_state:
        load.wait()

    up, down, other = tensor(1, 0), tensor(3, 0), tensor(0, 1)

    def gather(n, slot, to, h, part=None):
        if part is None:
            at = weights.at[slot, :, halves[h]]
        else:
            at = weights.at[slot, :, pl.ds(h * half + part * quarter, quarter)]
        return remote(at, at, gs_sem.at[h, n], gr_sem.at[h, n], (i, to))

    step_rows = 16

    def adam(h):
        cols = halves[h]

        def adam_step(k, carry):
            at = pl.ds(pl.multiple_of(k * step_rows, step_rows), step_rows)
            grad = prod[3, c, 1, at, cols].astype(F32) + pair[3, 1, at, cols].astype(F32)
            grad = grad + b_in[zl, at, cols].astype(F32) + b_in[2 + zl, at, cols].astype(F32)
            grad = grad + z_in[at, cols].astype(F32)
            master = state[0, at, cols]
            moment = BETA_ONE * state[1, at, cols] + (1.0 - BETA_ONE) * grad
            second = BETA_TWO * state[2, at, cols] + (1.0 - BETA_TWO) * grad * grad
            update = moment / CORRECT_ONE / (jnp.sqrt(second / CORRECT_TWO) + ADAM_EPS)
            master = master - LEARN_RATE * (update + DECAY * master)
            state[0, at, cols] = master
            state[1, at, cols] = moment
            state[2, at, cols] = second
            weights[t, at, cols] = master.astype(BF16)
            return carry

        lax.fori_loop(0, OWNED // step_rows, adam_step, 0)

    g_up, g_down, g_other = [], [], []
    for h in range(2):
        z_copies[h].wait_recv()
        adam(h)
        g_up.append(gather(0, t, up, h))
        g_down.append(gather(1, t, down, h))
        g_other.append(gather(2, t, other, h))
        g_other[h].start()
        g_up[h].start()
        g_down[h].start()
    point(3)

    outs = [
        pltpu.make_async_copy(state.at[k], ref, out_sem.at[k])
        for k, ref in enumerate((oma_h, omo_h, ose_h))
    ]
    for out in outs:
        out.start()

    last = []
    for h in range(2):
        g_up[h].wait_recv()
        last.append(gather(3, down, up, h, 0))
        last[-1].start()
        g_down[h].wait_recv()
        last.append(gather(4, up, down, h, 1))
        last[-1].start()
    point(4)
    o_up, o_down = [], []
    for h in range(2):
        g_other[h].wait_recv()
        o_up.append(gather(5, other, up, h))
        o_up[h].start()
        o_down.append(gather(6, other, down, h))
        o_down[h].start()
    point(5)
    for h in range(2):
        o_up[h].wait_recv()
        last.append(gather(7, tensor(3, 1), up, h, 0))
        last[-1].start()
        o_down[h].wait_recv()
        last.append(gather(8, tensor(1, 1), down, h, 1))
        last[-1].start()
    for copy in last:
        copy.wait_recv()
    out = pltpu.make_async_copy(weights, ohw_h, out_sem.at[3])
    out.start()
    outs.append(out)
    point(6)
    for copy in near_copies:
        copy.wait_recv()

    @pl.when(zl != c)
    def _():
        for copy in far_copies:
            copy.wait_recv()

    @pl.when(zl == c)
    def _():
        for copy in relay_copies:
            copy.wait_recv()
            copy.wait_send()

    for copy in started:
        copy.wait_send()
    for out in outs:
        out.wait()


def finish(own, ma, mo, se, hw, recv, oma_h, omo_h, ose_h, ohw_h, ocold_h, stage, out_sem, cold_sem):
    i = lax.axis_index("dp")
    width = recv.shape[-1]
    qlocal = width * CHUNKS
    outs = []

    def put(src, dst, sem):
        outs.append(pltpu.make_async_copy(src, dst, sem))
        outs[-1].start()

    for k, (src, dst) in enumerate(((ma, oma_h), (mo, omo_h), (se, ose_h))):
        put(src, dst, out_sem.at[k])
    for slot in range(8):
        put(hw.at[slot], ohw_h.at[:, pl.ds(slot * qlocal, qlocal)], out_sem.at[3 + slot])
    ones_prev, place_prev = slots(own, lax.rem(i + 15, 16))
    ones_next, place_next = slots(own, lax.rem(i + 1, 16))
    for n in range(CHUNKS):
        for k in range(COLD):
            a = recv[0, n, jnp.minimum(place_prev[k], SENT - 1)].astype(F32)
            b = recv[1, n, jnp.maximum(place_next[k] - 1, 0)].astype(F32)
            a = jnp.where(ones_prev[k] == 1, a, 0.0)
            b = jnp.where(ones_next[k] == 0, b, 0.0)
            stage[n, k * BLOCK : (k + 1) * BLOCK] = a + b
        put(stage.at[n], ocold_h.at[:, pl.ds(n * width, width)], cold_sem.at[n])
    for out in outs:
        out.wait()


def per_device(activations, out_grad, block_ids, owner_map, master, moment, second):
    rows, tokens, qlocal = activations.shape[0], out_grad.shape[0], out_grad.shape[1]
    width = qlocal // CHUNKS
    partners = len(OFFSETS)
    dma, like = pltpu.SemaphoreType.DMA, jax.ShapeDtypeStruct
    anywhere = pl.BlockSpec(memory_space=pl.ANY)
    hbm = pl.BlockSpec(memory_space=pltpu.HBM)
    smem = pl.BlockSpec(memory_space=pltpu.SMEM)
    vmem = pl.BlockSpec(memory_space=pltpu.VMEM)
    owners = owner_map.T
    chosen = pl.pallas_call(
        pick,
        name="pick",
        out_shape=(like((PARTS, 8, rows, 2 * BLOCK), BF16), like((8, rows, COLD * BLOCK), BF16)),
        in_specs=[smem, smem, hbm],
        out_specs=(vmem, vmem),
        scratch_shapes=[pltpu.VMEM((rows, D), BF16), dma],
        cost_estimate=pl.CostEstimate(flops=2000000000, bytes_accessed=3000000, transcendentals=0),
        compiler_params=pltpu.CompilerParams(vmem_limit_bytes=52 * 1024 * 1024),
    )(block_ids, owners, activations)
    states = (like(master.shape, F32),) * 3
    gathered = pl.pallas_call(
        exchange,
        name="exchange",
        out_shape=(
            *states,
            like((8, OWNED, qlocal), BF16),
            like((2, CHUNKS, SENT, BLOCK, width), BF16),
        ),
        in_specs=[anywhere] * 2 + [hbm] * 4,
        out_specs=(anywhere,) * 5,
        scratch_shapes=[
            pltpu.VMEM((tokens, qlocal), BF16),
            pltpu.VMEM((3, OWNED, qlocal), F32),
            pltpu.VMEM((PARTS, tokens, 2 * BLOCK), BF16),
            pltpu.VMEM((tokens, COLD * BLOCK), BF16),
            pltpu.VMEM((PARTS, 2, 2, OWNED, qlocal), BF16),
            pltpu.VMEM((PARTS, 2, OWNED, qlocal), BF16),
            pltpu.VMEM((6, OWNED, qlocal), BF16),
            pltpu.VMEM((2, OWNED, qlocal), BF16),
            pltpu.VMEM((4, OWNED, qlocal), BF16),
            pltpu.VMEM((OWNED, qlocal), BF16),
            pltpu.VMEM((OWNED, qlocal), BF16),
            pltpu.VMEM((8, OWNED, qlocal), BF16),
            pltpu.VMEM((CHUNKS, COLD, BLOCK, width), BF16),
            pltpu.VMEM((CHUNKS, SENT, BLOCK, width), BF16),
            dma((9,)),
            dma((4,)),
            *[dma((PARTS, partners))] * 2,
            *[dma((partners,))] * 2,
            *[dma((PARTS,))] * 2,
            *[dma((2,))] * 2,
            *[dma((6,))] * 2,
            *[dma((2,))] * 2,
            *[dma((CHUNKS,))] * 6,
            *[dma((2, 9))] * 2,
        ],
        compiler_params=pltpu.CompilerParams(
            collective_id=0, has_side_effects=True, vmem_limit_bytes=40 * 1024 * 1024
        ),
    )(*chosen, out_grad, master, moment, second)
    return pl.pallas_call(
        finish,
        name="finish",
        out_shape=(
            *states,
            like((OWNED, 8 * qlocal), BF16),
            like((COLD * BLOCK, qlocal), F32),
        ),
        in_specs=[smem] + [vmem] * 5,
        out_specs=(anywhere,) * 5,
        scratch_shapes=[
            pltpu.VMEM((CHUNKS, COLD * BLOCK, width), F32),
            dma((11,)),
            dma((CHUNKS,)),
        ],
        compiler_params=pltpu.CompilerParams(vmem_limit_bytes=24 * 1024 * 1024),
    )(owners, *gathered)


def solution(mesh):
    return jax.shard_map(
        per_device,
        mesh=mesh,
        in_specs=(
            P(("dp", "tensor"), None),
            P("dp", "tensor"),
            P(),
            P(),
            P("dp", "tensor"),
            P("dp", "tensor"),
            P("dp", "tensor"),
        ),
        out_specs=(
            P("dp", "tensor"),
            P("dp", "tensor"),
            P("dp", "tensor"),
            P("dp", None),
            P("dp", "tensor"),
        ),
        check_vma=False,
    )
```

```python
import jax
import jax.numpy as jnp
from jax import lax
from jax.experimental import pallas as pl
from jax.experimental.pallas import tpu as pltpu
from jax.sharding import PartitionSpec as P

D = 16384
BLOCK = 128
HOT = 8
COLD = 4
SENT = 3
OWNED = 64
PARTS = 4
ORDER = (0, None, 1, 2, 3)
CHUNKS = 8
DIRECT = (0, 0, 2, 8, 8, 8, 8)
DIAGONAL = (8, 8, 8, 8, 8, 8, 8)
RELAYED = (0, 4, 6, 8, 8, 8, 8)

BETA_ONE = 0.9
BETA_TWO = 0.95
ADAM_EPS = 1e-08
LEARN_RATE = 0.01
DECAY = 0.1
CORRECT_ONE = 1.0 - 0.9**10
CORRECT_TWO = 1.0 - 0.95**10

OFFSETS = ((2, 1), (1, 1), (3, 1), (0, 1), (2, 0), (1, 0), (3, 0))
CONTRACT = (((1,), (0,)), ((), ()))
F32 = jnp.float32
BF16 = jnp.bfloat16


def place(i):
    return lax.div(i, 4), lax.rem(lax.div(i, 2), 2), lax.rem(i, 2)


def hot_block(k, x, zl):
    step = (2, 2, 1, 1, 3, 3, 0, 0)[k]
    side = (0, 1, 0, 1, 0, 1, 1 - zl, zl)[k]
    return lax.rem(x + step, 4) * 2 + side


def slots(own, index):
    ones = [own[k, index] for k in range(COLD)]
    seen, places = jnp.int32(0), []
    for k in range(COLD):
        places.append(seen)
        seen = seen + ones[k]
    places = [jnp.where(ones[k] == 1, places[k], seen + k - places[k]) for k in range(COLD)]
    return ones, places


def pick(ids, own, act_h, hot, cold, act, sem):
    load = pltpu.make_async_copy(act_h, act, sem)
    load.start()
    i = lax.axis_index("dp")
    x, zl, _ = place(i)
    _, mine = slots(own, i)
    load.wait()

    def columns(block):
        return act[:, pl.ds(pl.multiple_of(block * BLOCK, BLOCK), BLOCK)]

    def group_step(group, carry):
        for k in range(HOT):
            at = k % 2 * BLOCK
            hot[k // 2, group, :, at : at + BLOCK] = columns(ids[group, hot_block(k, x, zl)])
        for slot in range(COLD):
            block = jnp.int32(0)
            for k in range(COLD):
                block = block + jnp.where(mine[k] == slot, ids[group, HOT + k], 0)
            cold[group, :, slot * BLOCK : (slot + 1) * BLOCK] = columns(block)
        return carry

    lax.fori_loop(0, cold.shape[0], group_step, 0)


def exchange(
    send_hot, send_cold, og_h, ma_h, mo_h, se_h,
    oma_h, omo_h, ose_h, ohw_h, recv_h,
    og, state, hot_in, cold_in, prod, pair, quads, a_in, b_in, z_out, z_in, weights, parts, relay,
    load_sem, out_sem, hs_sem, hr_sem, cs_sem, cr_sem, ds_sem, dr_sem, as_sem, ar_sem,
    bs_sem, br_sem, zs_sem, zr_sem, ns_sem, nr_sem, fs_sem, fr_sem, xs_sem, xr_sem,
    gs_sem, gr_sem,
):
    rows, qlocal = send_hot.shape[2], og.shape[1]
    width, half, quarter = qlocal // CHUNKS, qlocal // 2, qlocal // 4
    i = lax.axis_index("dp")
    t = lax.axis_index("tensor")
    x, zl, c = place(i)
    y, zh = lax.div(t, 2), lax.rem(t, 2)

    def device(x_, zl_, c_):
        return ((x_ * 2 + zl_) * 2 + c_, t)

    def tensor(dy, dz):
        return lax.rem(y + dy, 4) * 2 + lax.rem(zh + dz, 2)

    right, left = device(lax.rem(x + 1, 4), zl, c), device(lax.rem(x + 3, 4), zl, c)
    mate, across = device(x, zl, 1 - c), device(x, 1 - zl, c)
    corner = device(x, 1 - zl, 1 - c)

    started = []

    def remote(src, dst, send, recv, to):
        copy = pltpu.make_async_remote_copy(
            src_ref=src, dst_ref=dst, send_sem=send, recv_sem=recv, device_id=to,
            device_id_type=pl.DeviceIdType.MESH,
        )
        started.append(copy)
        return copy

    own_rows = pl.ds(pl.multiple_of(t * rows, rows), rows)
    load_og = pltpu.make_async_copy(og_h, og, load_sem.at[0])
    load_own = [
        pltpu.make_async_copy(send_hot.at[p, t], hot_in.at[p, own_rows], load_sem.at[1 + p])
        for p in range(PARTS)
    ]
    load_cold = pltpu.make_async_copy(send_cold.at[t], cold_in.at[own_rows], load_sem.at[5])
    load_state = [
        pltpu.make_async_copy(ref, state.at[k], load_sem.at[6 + k])
        for k, ref in enumerate((ma_h, mo_h, se_h))
    ]
    for load in (load_og, *load_own, load_cold, *load_state):
        load.start()

    barrier = pltpu.get_barrier_semaphore()
    peers = [(i, tensor(dy, dz)) for dy, dz in OFFSETS] + [right, left, mate, across, corner]
    for peer in peers:
        pl.semaphore_signal(barrier, inc=1, device_id=peer, device_id_type=pl.DeviceIdType.MESH)
    pl.semaphore_wait(barrier, len(peers))

    hot_copies, cold_copies = [[] for _ in range(PARTS)], []
    for p in ORDER:
        for n, offset in enumerate(OFFSETS):
            to = tensor(*offset)
            if p is None:
                src, dst = send_cold.at[to], cold_in.at[own_rows]
                copy = remote(src, dst, cs_sem.at[n], cr_sem.at[n], (i, to))
                cold_copies.append(copy)
            else:
                src, dst = send_hot.at[p, to], hot_in.at[p, own_rows]
                copy = remote(src, dst, hs_sem.at[p, n], hr_sem.at[p, n], (i, to))
                hot_copies[p].append(copy)
            copy.start()

    mate_copies = [
        remote(prod.at[p, 1 - c], pair.at[p], ds_sem.at[p], dr_sem.at[p], mate)
        for p in range(PARTS)
    ]

    def multiply(p):
        load_own[p].wait()
        for copy in hot_copies[p]:
            copy.wait_recv()
        picked = hot_in[p].T
        for n in range(4):
            cols = pl.ds(n * quarter, quarter)
            got = lax.dot_general(picked, og[:, cols], CONTRACT, preferred_element_type=F32)
            got = got.astype(BF16)
            for k in range(2):
                for core in range(2):
                    at = k * BLOCK + core * OWNED
                    prod[p, core, k, :, cols] = got[at : at + OWNED]
        mate_copies[p].start()

    def pair_sum(k, cols):
        p, k = k // 2, k % 2
        return prod[p, c, k, :, cols].astype(F32) + pair[p, k, :, cols].astype(F32)

    every = pl.ds(0, qlocal)
    halves = [pl.ds(h * half, half) for h in range(2)]
    a_right = remote(quads.at[0], a_in.at[0], as_sem.at[0], ar_sem.at[0], right)
    a_left = remote(quads.at[1], a_in.at[1], as_sem.at[1], ar_sem.at[1], left)
    b_right = remote(quads.at[3], b_in.at[1], bs_sem.at[0], br_sem.at[0], right)
    b_left = remote(quads.at[4], b_in.at[2], bs_sem.at[1], br_sem.at[1], left)
    m_right = [
        remote(
            quads.at[2, :, cols], b_in.at[0, :, cols], bs_sem.at[2 + h], br_sem.at[2 + h], right
        )
        for h, cols in enumerate(halves)
    ]
    m_left = [
        remote(quads.at[5, :, cols], b_in.at[3, :, cols], bs_sem.at[4 + h], br_sem.at[4 + h], left)
        for h, cols in enumerate(halves)
    ]

    near_copies = [
        remote(parts.at[n, pl.ds(c, SENT)], recv_h.at[c, n], ns_sem.at[n], nr_sem.at[n], mate)
        for n in range(CHUNKS)
    ]
    far_copies = [
        remote(
            parts.at[n, pl.ds(1 - c, SENT)], recv_h.at[1 - c, n], fs_sem.at[n], fr_sem.at[n], corner
        )
        for n in range(CHUNKS)
    ]
    lift_copies = [
        remote(parts.at[n, pl.ds(1 - c, SENT)], relay.at[n], fs_sem.at[n], fr_sem.at[n], corner)
        for n in range(CHUNKS)
    ]
    onward = device(lax.rem(x + 1 + 2 * c, 4), zl, c)
    relay_copies = [
        remote(relay.at[n], recv_h.at[c, n], xs_sem.at[n], xr_sem.at[n], onward)
        for n in range(CHUNKS)
    ]
    del started[-2 * CHUNKS :]

    def send_far(direct, first, last):
        if first < last:

            @pl.when(zl != c if direct else zl == c)
            def _():
                for n in range(first, last):
                    (far_copies if direct else lift_copies)[n].start()

    def point(k):
        if RELAYED[k - 1] < RELAYED[k]:

            @pl.when(zl == c)
            def _():
                for n in range(RELAYED[k - 1], RELAYED[k]):
                    lift_copies[n].wait_recv()
                    relay_copies[n].start()

        send_far(True, DIRECT[k - 1], DIRECT[k])
        send_far(False, DIAGONAL[k - 1], DIAGONAL[k])

    def cold_products():
        load_cold.wait()
        for copy in cold_copies:
            copy.wait_recv()
        picked = cold_in[...].T
        for n in range(CHUNKS):
            cols = pl.ds(n * width, width)
            got = lax.dot_general(picked, og[:, cols], CONTRACT, preferred_element_type=F32)
            parts[n] = got.astype(BF16).reshape(COLD, BLOCK, width)
            if n < DIRECT[0]:
                send_far(True, n, n + 1)
            if n < DIAGONAL[0]:
                send_far(False, n, n + 1)

    load_og.wait()
    multiply(0)
    cold_products()
    multiply(1)
    mate_copies[0].wait_recv()
    quads[0] = pair_sum(0, every).astype(BF16)
    a_right.start()
    quads[1] = pair_sum(1, every).astype(BF16)
    a_left.start()
    multiply(2)
    mate_copies[1].wait_recv()
    quads[3] = pair_sum(3, every).astype(BF16)
    b_right.start()
    mate_copies[2].wait_recv()
    quads[4] = pair_sum(4, every).astype(BF16)
    b_left.start()
    multiply(3)

    a_right.wait_recv()
    for h, cols in enumerate(halves):
        quads[2, :, cols] = (pair_sum(2, cols) + a_in[0, :, cols].astype(F32)).astype(BF16)
        m_right[h].start()
        if h == 0:
            a_left.wait_recv()
        quads[5, :, cols] = (pair_sum(5, cols) + a_in[1, :, cols].astype(F32)).astype(BF16)
        m_left[h].start()
    point(1)
    for n in range(CHUNKS):
        near_copies[n].start()

    z_copies = [
        remote(z_out.at[:, cols], z_in.at[:, cols], zs_sem.at[h], zr_sem.at[h], across)
        for h, cols in enumerate(halves)
    ]
    mate_copies[3].wait_recv()
    b_right.wait_recv()
    b_left.wait_recv()
    for h, cols in enumerate(halves):
        m_right[h].wait_recv()
        m_left[h].wait_recv()
        total = b_in[1 - zl, :, cols].astype(F32) + b_in[3 - zl, :, cols].astype(F32)
        z_out[:, cols] = (pair_sum(6, cols) + total).astype(BF16)
        z_copies[h].start()
    point(2)
    for load in load_state:
        load.wait()

    up, down, other = tensor(1, 0), tensor(3, 0), tensor(0, 1)

    def gather(n, slot, to, h, part=None):
        if part is None:
            at = weights.at[slot, :, halves[h]]
        else:
            at = weights.at[slot, :, pl.ds(h * half + part * quarter, quarter)]
        return remote(at, at, gs_sem.at[h, n], gr_sem.at[h, n], (i, to))

    step_rows = 16

    def adam(h):
        cols = halves[h]

        def adam_step(k, carry):
            at = pl.ds(pl.multiple_of(k * step_rows, step_rows), step_rows)
            grad = prod[3, c, 1, at, cols].astype(F32) + pair[3, 1, at, cols].astype(F32)
            grad = grad + b_in[zl, at, cols].astype(F32) + b_in[2 + zl, at, cols].astype(F32)
            grad = grad + z_in[at, cols].astype(F32)
            master = state[0, at, cols]
            moment = BETA_ONE * state[1, at, cols] + (1.0 - BETA_ONE) * grad
            second = BETA_TWO * state[2, at, cols] + (1.0 - BETA_TWO) * grad * grad
            update = moment / CORRECT_ONE / (jnp.sqrt(second / CORRECT_TWO) + ADAM_EPS)
            master = master - LEARN_RATE * (update + DECAY * master)
            state[0, at, cols] = master
            state[1, at, cols] = moment
            state[2, at, cols] = second
            weights[t, at, cols] = master.astype(BF16)
            return carry

        lax.fori_loop(0, OWNED // step_rows, adam_step, 0)

    g_up, g_down, g_other = [], [], []
    for h in range(2):
        z_copies[h].wait_recv()
        adam(h)
        g_up.append(gather(0, t, up, h))
        g_down.append(gather(1, t, down, h))
        g_other.append(gather(2, t, other, h))
        g_other[h].start()
        g_up[h].start()
        g_down[h].start()
    point(3)

    outs = [
        pltpu.make_async_copy(state.at[k], ref, out_sem.at[k])
        for k, ref in enumerate((oma_h, omo_h, ose_h))
    ]
    for out in outs:
        out.start()

    last = []
    for h in range(2):
        g_up[h].wait_recv()
        last.append(gather(3, down, up, h, 0))
        last[-1].start()
        g_down[h].wait_recv()
        last.append(gather(4, up, down, h, 1))
        last[-1].start()
    point(4)
    o_up, o_down = [], []
    for h in range(2):
        g_other[h].wait_recv()
        o_up.append(gather(5, other, up, h))
        o_up[h].start()
        o_down.append(gather(6, other, down, h))
        o_down[h].start()
    point(5)
    for h in range(2):
        o_up[h].wait_recv()
        last.append(gather(7, tensor(3, 1), up, h, 0))
        last[-1].start()
        o_down[h].wait_recv()
        last.append(gather(8, tensor(1, 1), down, h, 1))
        last[-1].start()
    for copy in last:
        copy.wait_recv()
    out = pltpu.make_async_copy(weights, ohw_h, out_sem.at[3])
    out.start()
    outs.append(out)
    point(6)
    for copy in near_copies:
        copy.wait_recv()

    @pl.when(zl != c)
    def _():
        for copy in far_copies:
            copy.wait_recv()

    @pl.when(zl == c)
    def _():
        for copy in relay_copies:
            copy.wait_recv()
            copy.wait_send()

    for copy in started:
        copy.wait_send()
    for out in outs:
        out.wait()


def finish(own, ma, mo, se, hw, recv, oma_h, omo_h, ose_h, ohw_h, ocold_h, stage, out_sem, cold_sem):
    i = lax.axis_index("dp")
    width = recv.shape[-1]
    qlocal = width * CHUNKS
    outs = []

    def put(src, dst, sem):
        outs.append(pltpu.make_async_copy(src, dst, sem))
        outs[-1].start()

    for k, (src, dst) in enumerate(((ma, oma_h), (mo, omo_h), (se, ose_h))):
        put(src, dst, out_sem.at[k])
    for slot in range(8):
        put(hw.at[slot], ohw_h.at[:, pl.ds(slot * qlocal, qlocal)], out_sem.at[3 + slot])
    ones_prev, place_prev = slots(own, lax.rem(i + 15, 16))
    ones_next, place_next = slots(own, lax.rem(i + 1, 16))
    for n in range(CHUNKS):
        for k in range(COLD):
            a = recv[0, n, jnp.minimum(place_prev[k], SENT - 1)].astype(F32)
            b = recv[1, n, jnp.maximum(place_next[k] - 1, 0)].astype(F32)
            a = jnp.where(ones_prev[k] == 1, a, 0.0)
            b = jnp.where(ones_next[k] == 0, b, 0.0)
            stage[n, k * BLOCK : (k + 1) * BLOCK] = a + b
        put(stage.at[n], ocold_h.at[:, pl.ds(n * width, width)], cold_sem.at[n])
    for out in outs:
        out.wait()


def per_device(activations, out_grad, block_ids, owner_map, master, moment, second):
    rows, tokens, qlocal = activations.shape[0], out_grad.shape[0], out_grad.shape[1]
    width = qlocal // CHUNKS
    partners = len(OFFSETS)
    dma, like = pltpu.SemaphoreType.DMA, jax.ShapeDtypeStruct
    anywhere = pl.BlockSpec(memory_space=pl.ANY)
    hbm = pl.BlockSpec(memory_space=pltpu.HBM)
    smem = pl.BlockSpec(memory_space=pltpu.SMEM)
    vmem = pl.BlockSpec(memory_space=pltpu.VMEM)
    owners = owner_map.T
    chosen = pl.pallas_call(
        pick,
        name="pick",
        out_shape=(like((PARTS, 8, rows, 2 * BLOCK), BF16), like((8, rows, COLD * BLOCK), BF16)),
        in_specs=[smem, smem, hbm],
        out_specs=(vmem, vmem),
        scratch_shapes=[pltpu.VMEM((rows, D), BF16), dma],
        cost_estimate=pl.CostEstimate(flops=2000000000, bytes_accessed=3000000, transcendentals=0),
        compiler_params=pltpu.CompilerParams(vmem_limit_bytes=52 * 1024 * 1024),
    )(block_ids, owners, activations)
    states = (like(master.shape, F32),) * 3
    gathered = pl.pallas_call(
        exchange,
        name="exchange",
        out_shape=(
            *states,
            like((8, OWNED, qlocal), BF16),
            like((2, CHUNKS, SENT, BLOCK, width), BF16),
        ),
        in_specs=[anywhere] * 2 + [hbm] * 4,
        out_specs=(anywhere,) * 5,
        scratch_shapes=[
            pltpu.VMEM((tokens, qlocal), BF16),
            pltpu.VMEM((3, OWNED, qlocal), F32),
            pltpu.VMEM((PARTS, tokens, 2 * BLOCK), BF16),
            pltpu.VMEM((tokens, COLD * BLOCK), BF16),
            pltpu.VMEM((PARTS, 2, 2, OWNED, qlocal), BF16),
            pltpu.VMEM((PARTS, 2, OWNED, qlocal), BF16),
            pltpu.VMEM((6, OWNED, qlocal), BF16),
            pltpu.VMEM((2, OWNED, qlocal), BF16),
            pltpu.VMEM((4, OWNED, qlocal), BF16),
            pltpu.VMEM((OWNED, qlocal), BF16),
            pltpu.VMEM((OWNED, qlocal), BF16),
            pltpu.VMEM((8, OWNED, qlocal), BF16),
            pltpu.VMEM((CHUNKS, COLD, BLOCK, width), BF16),
            pltpu.VMEM((CHUNKS, SENT, BLOCK, width), BF16),
            dma((9,)),
            dma((4,)),
            *[dma((PARTS, partners))] * 2,
            *[dma((partners,))] * 2,
            *[dma((PARTS,))] * 2,
            *[dma((2,))] * 2,
            *[dma((6,))] * 2,
            *[dma((2,))] * 2,
            *[dma((CHUNKS,))] * 6,
            *[dma((2, 9))] * 2,
        ],
        compiler_params=pltpu.CompilerParams(
            collective_id=0, has_side_effects=True, vmem_limit_bytes=40 * 1024 * 1024
        ),
    )(*chosen, out_grad, master, moment, second)
    return pl.pallas_call(
        finish,
        name="finish",
        out_shape=(
            *states,
            like((OWNED, 8 * qlocal), BF16),
            like((COLD * BLOCK, qlocal), F32),
        ),
        in_specs=[smem] + [vmem] * 5,
        out_specs=(anywhere,) * 5,
        scratch_shapes=[
            pltpu.VMEM((CHUNKS, COLD * BLOCK, width), F32),
            dma((11,)),
            dma((CHUNKS,)),
        ],
        compiler_params=pltpu.CompilerParams(vmem_limit_bytes=24 * 1024 * 1024),
    )(owners, *gathered)


def solution(mesh):
    return jax.shard_map(
        per_device,
        mesh=mesh,
        in_specs=(
            P(("dp", "tensor"), None),
            P("dp", "tensor"),
            P(),
            P(),
            P("dp", "tensor"),
            P("dp", "tensor"),
            P("dp", "tensor"),
        ),
        out_specs=(
            P("dp", "tensor"),
            P("dp", "tensor"),
            P("dp", "tensor"),
            P("dp", None),
            P("dp", "tensor"),
        ),
        check_vma=False,
    )
```

```python
import jax
import jax.numpy as jnp
from jax import lax
from jax.experimental import pallas as pl
from jax.experimental.pallas import tpu as pltpu
from jax.sharding import PartitionSpec as P

D = 16384
BLOCK = 128
HOT = 8
COLD = 4
SENT = 3
OWNED = 64
PARTS = 4
ORDER = (0, None, 1, 2, 3)
CHUNKS = 8
DIRECT = (0, 0, 2, 8, 8, 8, 8)
DIAGONAL = (8, 8, 8, 8, 8, 8, 8)
RELAYED = (0, 2, 4, 6, 8, 8, 8)

BETA_ONE = 0.9
BETA_TWO = 0.95
ADAM_EPS = 1e-08
LEARN_RATE = 0.01
DECAY = 0.1
CORRECT_ONE = 1.0 - 0.9**10
CORRECT_TWO = 1.0 - 0.95**10

OFFSETS = ((2, 1), (1, 1), (3, 1), (0, 1), (2, 0), (1, 0), (3, 0))
CONTRACT = (((1,), (0,)), ((), ()))
F32 = jnp.float32
BF16 = jnp.bfloat16


def place(i):
    return lax.div(i, 4), lax.rem(lax.div(i, 2), 2), lax.rem(i, 2)


def hot_block(k, x, zl):
    step = (2, 2, 1, 1, 3, 3, 0, 0)[k]
    side = (0, 1, 0, 1, 0, 1, 1 - zl, zl)[k]
    return lax.rem(x + step, 4) * 2 + side


def slots(own, index):
    ones = [own[k, index] for k in range(COLD)]
    seen, places = jnp.int32(0), []
    for k in range(COLD):
        places.append(seen)
        seen = seen + ones[k]
    places = [jnp.where(ones[k] == 1, places[k], seen + k - places[k]) for k in range(COLD)]
    return ones, places


def pick(ids, own, act_h, hot, cold, act, sem):
    load = pltpu.make_async_copy(act_h, act, sem)
    load.start()
    i = lax.axis_index("dp")
    x, zl, _ = place(i)
    _, mine = slots(own, i)
    load.wait()

    def columns(block):
        return act[:, pl.ds(pl.multiple_of(block * BLOCK, BLOCK), BLOCK)]

    def group_step(group, carry):
        for k in range(HOT):
            at = k % 2 * BLOCK
            hot[k // 2, group, :, at : at + BLOCK] = columns(ids[group, hot_block(k, x, zl)])
        for slot in range(COLD):
            block = jnp.int32(0)
            for k in range(COLD):
                block = block + jnp.where(mine[k] == slot, ids[group, HOT + k], 0)
            cold[group, :, slot * BLOCK : (slot + 1) * BLOCK] = columns(block)
        return carry

    lax.fori_loop(0, cold.shape[0], group_step, 0)


def exchange(
    send_hot, send_cold, og_h, ma_h, mo_h, se_h,
    oma_h, omo_h, ose_h, ohw_h, recv_h,
    og, state, hot_in, cold_in, prod, pair, quads, a_in, b_in, z_out, z_in, weights, parts, relay,
    load_sem, out_sem, hs_sem, hr_sem, cs_sem, cr_sem, ds_sem, dr_sem, as_sem, ar_sem,
    bs_sem, br_sem, zs_sem, zr_sem, ns_sem, nr_sem, fs_sem, fr_sem, xs_sem, xr_sem,
    gs_sem, gr_sem,
):
    rows, qlocal = send_hot.shape[2], og.shape[1]
    width, half, quarter = qlocal // CHUNKS, qlocal // 2, qlocal // 4
    i = lax.axis_index("dp")
    t = lax.axis_index("tensor")
    x, zl, c = place(i)
    y, zh = lax.div(t, 2), lax.rem(t, 2)

    def device(x_, zl_, c_):
        return ((x_ * 2 + zl_) * 2 + c_, t)

    def tensor(dy, dz):
        return lax.rem(y + dy, 4) * 2 + lax.rem(zh + dz, 2)

    right, left = device(lax.rem(x + 1, 4), zl, c), device(lax.rem(x + 3, 4), zl, c)
    mate, across = device(x, zl, 1 - c), device(x, 1 - zl, c)
    corner = device(x, 1 - zl, 1 - c)

    started = []

    def remote(src, dst, send, recv, to):
        copy = pltpu.make_async_remote_copy(
            src_ref=src, dst_ref=dst, send_sem=send, recv_sem=recv, device_id=to,
            device_id_type=pl.DeviceIdType.MESH,
        )
        started.append(copy)
        return copy

    own_rows = pl.ds(pl.multiple_of(t * rows, rows), rows)
    load_og = pltpu.make_async_copy(og_h, og, load_sem.at[0])
    load_own = [
        pltpu.make_async_copy(send_hot.at[p, t], hot_in.at[p, own_rows], load_sem.at[1 + p])
        for p in range(PARTS)
    ]
    load_cold = pltpu.make_async_copy(send_cold.at[t], cold_in.at[own_rows], load_sem.at[5])
    load_state = [
        pltpu.make_async_copy(ref, state.at[k], load_sem.at[6 + k])
        for k, ref in enumerate((ma_h, mo_h, se_h))
    ]
    for load in (load_og, *load_own, load_cold, *load_state):
        load.start()

    barrier = pltpu.get_barrier_semaphore()
    peers = [(i, tensor(dy, dz)) for dy, dz in OFFSETS] + [right, left, mate, across, corner]
    for peer in peers:
        pl.semaphore_signal(barrier, inc=1, device_id=peer, device_id_type=pl.DeviceIdType.MESH)
    pl.semaphore_wait(barrier, len(peers))

    hot_copies, cold_copies = [[] for _ in range(PARTS)], []
    for p in ORDER:
        for n, offset in enumerate(OFFSETS):
            to = tensor(*offset)
            if p is None:
                src, dst = send_cold.at[to], cold_in.at[own_rows]
                copy = remote(src, dst, cs_sem.at[n], cr_sem.at[n], (i, to))
                cold_copies.append(copy)
            else:
                src, dst = send_hot.at[p, to], hot_in.at[p, own_rows]
                copy = remote(src, dst, hs_sem.at[p, n], hr_sem.at[p, n], (i, to))
                hot_copies[p].append(copy)
            copy.start()

    mate_copies = [
        remote(prod.at[p, 1 - c], pair.at[p], ds_sem.at[p], dr_sem.at[p], mate)
        for p in range(PARTS)
    ]

    def multiply(p):
        load_own[p].wait()
        for copy in hot_copies[p]:
            copy.wait_recv()
        picked = hot_in[p].T
        for n in range(4):
            cols = pl.ds(n * quarter, quarter)
            got = lax.dot_general(picked, og[:, cols], CONTRACT, preferred_element_type=F32)
            got = got.astype(BF16)
            for k in range(2):
                for core in range(2):
                    at = k * BLOCK + core * OWNED
                    prod[p, core, k, :, cols] = got[at : at + OWNED]
        mate_copies[p].start()

    def pair_sum(k, cols):
        p, k = k // 2, k % 2
        return prod[p, c, k, :, cols].astype(F32) + pair[p, k, :, cols].astype(F32)

    every = pl.ds(0, qlocal)
    halves = [pl.ds(h * half, half) for h in range(2)]
    a_right = remote(quads.at[0], a_in.at[0], as_sem.at[0], ar_sem.at[0], right)
    a_left = remote(quads.at[1], a_in.at[1], as_sem.at[1], ar_sem.at[1], left)
    b_right = remote(quads.at[3], b_in.at[1], bs_sem.at[0], br_sem.at[0], right)
    b_left = remote(quads.at[4], b_in.at[2], bs_sem.at[1], br_sem.at[1], left)
    m_right = [
        remote(
            quads.at[2, :, cols], b_in.at[0, :, cols], bs_sem.at[2 + h], br_sem.at[2 + h], right
        )
        for h, cols in enumerate(halves)
    ]
    m_left = [
        remote(quads.at[5, :, cols], b_in.at[3, :, cols], bs_sem.at[4 + h], br_sem.at[4 + h], left)
        for h, cols in enumerate(halves)
    ]

    near_copies = [
        remote(parts.at[n, pl.ds(c, SENT)], recv_h.at[c, n], ns_sem.at[n], nr_sem.at[n], mate)
        for n in range(CHUNKS)
    ]
    far_copies = [
        remote(
            parts.at[n, pl.ds(1 - c, SENT)], recv_h.at[1 - c, n], fs_sem.at[n], fr_sem.at[n], corner
        )
        for n in range(CHUNKS)
    ]
    lift_copies = [
        remote(parts.at[n, pl.ds(1 - c, SENT)], relay.at[n], fs_sem.at[n], fr_sem.at[n], corner)
        for n in range(CHUNKS)
    ]
    onward = device(lax.rem(x + 1 + 2 * c, 4), zl, c)
    relay_copies = [
        remote(relay.at[n], recv_h.at[c, n], xs_sem.at[n], xr_sem.at[n], onward)
        for n in range(CHUNKS)
    ]
    del started[-2 * CHUNKS :]

    def send_far(direct, first, last):
        if first < last:

            @pl.when(zl != c if direct else zl == c)
            def _():
                for n in range(first, last):
                    (far_copies if direct else lift_copies)[n].start()

    def point(k):
        if RELAYED[k - 1] < RELAYED[k]:

            @pl.when(zl == c)
            def _():
                for n in range(RELAYED[k - 1], RELAYED[k]):
                    lift_copies[n].wait_recv()
                    relay_copies[n].start()

        send_far(True, DIRECT[k - 1], DIRECT[k])
        send_far(False, DIAGONAL[k - 1], DIAGONAL[k])

    def cold_products():
        load_cold.wait()
        for copy in cold_copies:
            copy.wait_recv()
        picked = cold_in[...].T
        for n in range(CHUNKS):
            cols = pl.ds(n * width, width)
            got = lax.dot_general(picked, og[:, cols], CONTRACT, preferred_element_type=F32)
            parts[n] = got.astype(BF16).reshape(COLD, BLOCK, width)
            if n < DIRECT[0]:
                send_far(True, n, n + 1)
            if n < DIAGONAL[0]:
                send_far(False, n, n + 1)

    load_og.wait()
    multiply(0)
    cold_products()
    multiply(1)
    mate_copies[0].wait_recv()
    quads[0] = pair_sum(0, every).astype(BF16)
    a_right.start()
    quads[1] = pair_sum(1, every).astype(BF16)
    a_left.start()
    multiply(2)
    mate_copies[1].wait_recv()
    quads[3] = pair_sum(3, every).astype(BF16)
    b_right.start()
    mate_copies[2].wait_recv()
    quads[4] = pair_sum(4, every).astype(BF16)
    b_left.start()
    multiply(3)

    a_right.wait_recv()
    for h, cols in enumerate(halves):
        quads[2, :, cols] = (pair_sum(2, cols) + a_in[0, :, cols].astype(F32)).astype(BF16)
        m_right[h].start()
        if h == 0:
            a_left.wait_recv()
        quads[5, :, cols] = (pair_sum(5, cols) + a_in[1, :, cols].astype(F32)).astype(BF16)
        m_left[h].start()
    point(1)
    for n in range(CHUNKS):
        near_copies[n].start()

    z_copies = [
        remote(z_out.at[:, cols], z_in.at[:, cols], zs_sem.at[h], zr_sem.at[h], across)
        for h, cols in enumerate(halves)
    ]
    mate_copies[3].wait_recv()
    b_right.wait_recv()
    b_left.wait_recv()
    for h, cols in enumerate(halves):
        m_right[h].wait_recv()
        m_left[h].wait_recv()
        total = b_in[1 - zl, :, cols].astype(F32) + b_in[3 - zl, :, cols].astype(F32)
        z_out[:, cols] = (pair_sum(6, cols) + total).astype(BF16)
        z_copies[h].start()
    point(2)
    for load in load_state:
        load.wait()

    up, down, other = tensor(1, 0), tensor(3, 0), tensor(0, 1)

    def gather(n, slot, to, h, part=None):
        if part is None:
            at = weights.at[slot, :, halves[h]]
        else:
            at = weights.at[slot, :, pl.ds(h * half + part * quarter, quarter)]
        return remote(at, at, gs_sem.at[h, n], gr_sem.at[h, n], (i, to))

    step_rows = 16

    def adam(h):
        cols = halves[h]

        def adam_step(k, carry):
            at = pl.ds(pl.multiple_of(k * step_rows, step_rows), step_rows)
            grad = prod[3, c, 1, at, cols].astype(F32) + pair[3, 1, at, cols].astype(F32)
            grad = grad + b_in[zl, at, cols].astype(F32) + b_in[2 + zl, at, cols].astype(F32)
            grad = grad + z_in[at, cols].astype(F32)
            master = state[0, at, cols]
            moment = BETA_ONE * state[1, at, cols] + (1.0 - BETA_ONE) * grad
            second = BETA_TWO * state[2, at, cols] + (1.0 - BETA_TWO) * grad * grad
            update = moment / CORRECT_ONE / (jnp.sqrt(second / CORRECT_TWO) + ADAM_EPS)
            master = master - LEARN_RATE * (update + DECAY * master)
            state[0, at, cols] = master
            state[1, at, cols] = moment
            state[2, at, cols] = second
            weights[t, at, cols] = master.astype(BF16)
            return carry

        lax.fori_loop(0, OWNED // step_rows, adam_step, 0)

    g_up, g_down, g_other = [], [], []
    for h in range(2):
        z_copies[h].wait_recv()
        adam(h)
        g_up.append(gather(0, t, up, h))
        g_down.append(gather(1, t, down, h))
        g_other.append(gather(2, t, other, h))
        g_other[h].start()
        g_up[h].start()
        g_down[h].start()
    point(3)

    outs = [
        pltpu.make_async_copy(state.at[k], ref, out_sem.at[k])
        for k, ref in enumerate((oma_h, omo_h, ose_h))
    ]
    for out in outs:
        out.start()

    last = []
    for h in range(2):
        g_up[h].wait_recv()
        last.append(gather(3, down, up, h, 0))
        last[-1].start()
        g_down[h].wait_recv()
        last.append(gather(4, up, down, h, 1))
        last[-1].start()
    point(4)
    o_up, o_down = [], []
    for h in range(2):
        g_other[h].wait_recv()
        o_up.append(gather(5, other, up, h))
        o_up[h].start()
        o_down.append(gather(6, other, down, h))
        o_down[h].start()
    point(5)
    for h in range(2):
        o_up[h].wait_recv()
        last.append(gather(7, tensor(3, 1), up, h, 0))
        last[-1].start()
        o_down[h].wait_recv()
        last.append(gather(8, tensor(1, 1), down, h, 1))
        last[-1].start()
    for copy in last:
        copy.wait_recv()
    out = pltpu.make_async_copy(weights, ohw_h, out_sem.at[3])
    out.start()
    outs.append(out)
    point(6)
    for copy in near_copies:
        copy.wait_recv()

    @pl.when(zl != c)
    def _():
        for copy in far_copies:
            copy.wait_recv()

    @pl.when(zl == c)
    def _():
        for copy in relay_copies:
            copy.wait_recv()
            copy.wait_send()

    for copy in started:
        copy.wait_send()
    for out in outs:
        out.wait()


def finish(own, ma, mo, se, hw, recv, oma_h, omo_h, ose_h, ohw_h, ocold_h, stage, out_sem, cold_sem):
    i = lax.axis_index("dp")
    width = recv.shape[-1]
    qlocal = width * CHUNKS
    outs = []

    def put(src, dst, sem):
        outs.append(pltpu.make_async_copy(src, dst, sem))
        outs[-1].start()

    for k, (src, dst) in enumerate(((ma, oma_h), (mo, omo_h), (se, ose_h))):
        put(src, dst, out_sem.at[k])
    for slot in range(8):
        put(hw.at[slot], ohw_h.at[:, pl.ds(slot * qlocal, qlocal)], out_sem.at[3 + slot])
    ones_prev, place_prev = slots(own, lax.rem(i + 15, 16))
    ones_next, place_next = slots(own, lax.rem(i + 1, 16))
    for n in range(CHUNKS):
        for k in range(COLD):
            a = recv[0, n, jnp.minimum(place_prev[k], SENT - 1)].astype(F32)
            b = recv[1, n, jnp.maximum(place_next[k] - 1, 0)].astype(F32)
            a = jnp.where(ones_prev[k] == 1, a, 0.0)
            b = jnp.where(ones_next[k] == 0, b, 0.0)
            stage[n, k * BLOCK : (k + 1) * BLOCK] = a + b
        put(stage.at[n], ocold_h.at[:, pl.ds(n * width, width)], cold_sem.at[n])
    for out in outs:
        out.wait()


def per_device(activations, out_grad, block_ids, owner_map, master, moment, second):
    rows, tokens, qlocal = activations.shape[0], out_grad.shape[0], out_grad.shape[1]
    width = qlocal // CHUNKS
    partners = len(OFFSETS)
    dma, like = pltpu.SemaphoreType.DMA, jax.ShapeDtypeStruct
    anywhere = pl.BlockSpec(memory_space=pl.ANY)
    hbm = pl.BlockSpec(memory_space=pltpu.HBM)
    smem = pl.BlockSpec(memory_space=pltpu.SMEM)
    vmem = pl.BlockSpec(memory_space=pltpu.VMEM)
    owners = owner_map.T
    chosen = pl.pallas_call(
        pick,
        name="pick",
        out_shape=(like((PARTS, 8, rows, 2 * BLOCK), BF16), like((8, rows, COLD * BLOCK), BF16)),
        in_specs=[smem, smem, hbm],
        out_specs=(vmem, vmem),
        scratch_shapes=[pltpu.VMEM((rows, D), BF16), dma],
        cost_estimate=pl.CostEstimate(flops=2000000000, bytes_accessed=3000000, transcendentals=0),
        compiler_params=pltpu.CompilerParams(vmem_limit_bytes=52 * 1024 * 1024),
    )(block_ids, owners, activations)
    states = (like(master.shape, F32),) * 3
    gathered = pl.pallas_call(
        exchange,
        name="exchange",
        out_shape=(
            *states,
            like((8, OWNED, qlocal), BF16),
            like((2, CHUNKS, SENT, BLOCK, width), BF16),
        ),
        in_specs=[anywhere] * 2 + [hbm] * 4,
        out_specs=(anywhere,) * 5,
        scratch_shapes=[
            pltpu.VMEM((tokens, qlocal), BF16),
            pltpu.VMEM((3, OWNED, qlocal), F32),
            pltpu.VMEM((PARTS, tokens, 2 * BLOCK), BF16),
            pltpu.VMEM((tokens, COLD * BLOCK), BF16),
            pltpu.VMEM((PARTS, 2, 2, OWNED, qlocal), BF16),
            pltpu.VMEM((PARTS, 2, OWNED, qlocal), BF16),
            pltpu.VMEM((6, OWNED, qlocal), BF16),
            pltpu.VMEM((2, OWNED, qlocal), BF16),
            pltpu.VMEM((4, OWNED, qlocal), BF16),
            pltpu.VMEM((OWNED, qlocal), BF16),
            pltpu.VMEM((OWNED, qlocal), BF16),
            pltpu.VMEM((8, OWNED, qlocal), BF16),
            pltpu.VMEM((CHUNKS, COLD, BLOCK, width), BF16),
            pltpu.VMEM((CHUNKS, SENT, BLOCK, width), BF16),
            dma((9,)),
            dma((4,)),
            *[dma((PARTS, partners))] * 2,
            *[dma((partners,))] * 2,
            *[dma((PARTS,))] * 2,
            *[dma((2,))] * 2,
            *[dma((6,))] * 2,
            *[dma((2,))] * 2,
            *[dma((CHUNKS,))] * 6,
            *[dma((2, 9))] * 2,
        ],
        compiler_params=pltpu.CompilerParams(
            collective_id=0, has_side_effects=True, vmem_limit_bytes=40 * 1024 * 1024
        ),
    )(*chosen, out_grad, master, moment, second)
    return pl.pallas_call(
        finish,
        name="finish",
        out_shape=(
            *states,
            like((OWNED, 8 * qlocal), BF16),
            like((COLD * BLOCK, qlocal), F32),
        ),
        in_specs=[smem] + [vmem] * 5,
        out_specs=(anywhere,) * 5,
        scratch_shapes=[
            pltpu.VMEM((CHUNKS, COLD * BLOCK, width), F32),
            dma((11,)),
            dma((CHUNKS,)),
        ],
        compiler_params=pltpu.CompilerParams(vmem_limit_bytes=24 * 1024 * 1024),
    )(owners, *gathered)


def solution(mesh):
    return jax.shard_map(
        per_device,
        mesh=mesh,
        in_specs=(
            P(("dp", "tensor"), None),
            P("dp", "tensor"),
            P(),
            P(),
            P("dp", "tensor"),
            P("dp", "tensor"),
            P("dp", "tensor"),
        ),
        out_specs=(
            P("dp", "tensor"),
            P("dp", "tensor"),
            P("dp", "tensor"),
            P("dp", None),
            P("dp", "tensor"),
        ),
        check_vma=False,
    )
```
